32 devices in a mesh: gx: 8 (over z, y), gy: 4 (over x, core).
Axes of the slice: x: 2, y: 2, z: 4, core: 2. Of those that a mesh axis runs over, the one named last changes fastest.
Arguments:
- preserved_vector: float32 [14, 64, 32, 128], P(None, 'gx', 'gy'), may hold values from -200 to 200, as said below
- nasa_table: float32 [32, 6], replicated, may hold values from -4 to 4.5, as said below
- gas_constant: float32 [32], replicated, may hold values from 0.3 to 3
- species_index: int32 [9], replicated, may hold values from 0 to 31, as said below
- face_kind: int32 [8, 4, 2], P('gx', 'gy'), may hold values from 0 to 1
Outputs:
- increment: float32 [14, 64, 32, 128], P(None, 'gx', 'gy')
The draws below stay inside these ranges and needn't reach their ends.
Inputs may be any that keep to these rules, and one draw needn't show every extreme that they name: `preserved_vector`: every cell is a physical state: positive partial densities and an energy whose temperature lies between 0.5 and 2.5. `nasa_table`: each row's cp over R polynomial exceeds 1.5 for temperatures 0.3 to 3. `species_index`: 9 distinct rows.
All inputs are finite; a program needn't handle non-finite values.
Results may differ from the reference program's by a relative error of at most 0.0003.
Values sent between devices are 32-bit elements; how exact they have to be, the bound alone decides.
A program may use at most 64 MiB of HBM per device.

```python
import math
import jax
import jax.numpy as jnp
from jax import lax

NS = 9
NVAR = 14
KINDS = 32
NEWTON = 2
CX = 8
CY = 8
NX = 64
NY = 32
NZ = 128
N_GX = 8
N_GY = 4


def thermo_tables(key):
    lower = jnp.array([2.5, 0.0, -0.05, -0.01, -0.002, -4.0], jnp.float32)
    upper = jnp.array([4.5, 0.6, 0.05, 0.01, 0.002, 4.0], jnp.float32)
    table = lower + (upper - lower) * jax.random.uniform(jax.random.fold_in(key, 101), (KINDS, 6), jnp.float32)
    gases = jnp.exp(jax.random.uniform(jax.random.fold_in(key, 102), (KINDS,), jnp.float32, math.log(0.3), math.log(3.0)))
    middle_rows = (jax.random.permutation(jax.random.fold_in(key, 103), KINDS - 2)[:NS - 2] + 1).astype(jnp.int32)
    end_rows = jnp.array([0, KINDS - 1], jnp.int32)
    pooled = jnp.concatenate([end_rows, middle_rows], axis=0)
    shuffle = jax.random.permutation(jax.random.fold_in(key, 104), NS).astype(jnp.int32)
    chosen = pooled[shuffle].astype(jnp.int32)
    return (table, gases, chosen)


def draw_nasa_table(key, part):
    return thermo_tables(key)[0]


def draw_gas_constant(key, part):
    return thermo_tables(key)[1]


def draw_species_index(key, part):
    return thermo_tables(key)[2]


def draw_preserved_vector(key, part):
    table, gases, chosen = thermo_tables(key)
    nasa_table_weights = table[chosen]
    component_kind_r_factor = gases[chosen]
    grid_sizes_list = (NX, NY, NZ)
    draw_seed_handles_list = [jax.random.fold_in(key, 200 + number) for number in range(6)]
    abscissa_place = (jnp.arange(NX, dtype=jnp.float32) / NX)[:, None, None]
    ordinate_place = (jnp.arange(NY, dtype=jnp.float32) / NY)[None, :, None]
    ramp = 0.3 + 1.35 * (abscissa_place + ordinate_place)
    bulk_compactness = jnp.exp(jax.random.uniform(draw_seed_handles_list[0], grid_sizes_list, jnp.float32, -0.4, 0.4))
    fractions = jax.nn.softmax(jax.random.normal(draw_seed_handles_list[1], (NS,) + grid_sizes_list, jnp.float32), axis=0)
    passive = jax.random.uniform(draw_seed_handles_list[2], grid_sizes_list, jnp.float32)
    kelvin_reading = jax.random.uniform(draw_seed_handles_list[3], grid_sizes_list, jnp.float32, 0.5, 2.4)
    velocity = 0.5 * ramp[None] * jnp.clip(jax.random.normal(draw_seed_handles_list[4], (3,) + grid_sizes_list, jnp.float32), -4.0, 4.0)
    prefix_addition_result = bulk_compactness[None] * fractions
    replicated_layer = kelvin_reading[None]
    columns = [nasa_table_weights[:, degree].reshape((NS, 1, 1, 1)) for degree in range(6)]
    chemical_heat_content = columns[5] + replicated_layer * (columns[0] + replicated_layer * (columns[1] / 2.0 + replicated_layer * (columns[2] / 3.0 + replicated_layer * (columns[3] / 4.0 + replicated_layer * columns[4] / 5.0))))
    caloric_tiers = component_kind_r_factor.reshape((NS, 1, 1, 1)) * (chemical_heat_content - replicated_layer)
    energy = jnp.sum(prefix_addition_result * caloric_tiers, axis=0) + 0.5 * bulk_compactness * jnp.sum(velocity * velocity, axis=0)
    return jnp.concatenate([prefix_addition_result, bulk_compactness[None] * velocity, energy[None], (bulk_compactness * passive)[None]], axis=0).astype(jnp.float32)


def set_ends(values, key, least, high):
    dims = values.shape
    index_at = [jax.random.randint(jax.random.fold_in(key, axis), (), 0, dims[axis]) for axis in range(len(dims))]
    values = values.at[tuple(index_at)].set(least)
    longest = dims.index(max(dims))
    index_at[longest] = (index_at[longest] + 1) % dims[longest]
    return values.at[tuple(index_at)].set(high)


def setup_inputs(seed: int = 0) -> dict:
    arg_keys = jax.random.split(jax.random.key(seed), 6)
    preserved_vector = draw_preserved_vector(jax.random.fold_in(arg_keys[5], 71), 0)
    nasa_table = draw_nasa_table(jax.random.fold_in(arg_keys[5], 71), 0)
    gas_constant = draw_gas_constant(jax.random.fold_in(arg_keys[5], 71), 0)
    species_index = draw_species_index(jax.random.fold_in(arg_keys[5], 71), 0)
    face_kind = set_ends(jax.random.randint(arg_keys[4], (N_GX, N_GY, 2), 0, 2), jax.random.fold_in(arg_keys[4], 1), 0, 1).astype(jnp.int32)
    return {"preserved_vector": preserved_vector, "nasa_table": nasa_table, "gas_constant": gas_constant, "species_index": species_index, "face_kind": face_kind}


EPSILON = 1e-06
COURANT = 0.8

def column(vector, trailing_sizes):
    return vector.reshape((vector.shape[0],) + (1,) * trailing_sizes)

def caloric_fitted_curves_table(nasa_table_weights, kelvin_reading):
    trailing_sizes = kelvin_reading.ndim
    columns = [column(nasa_table_weights[:, degree], trailing_sizes) for degree in range(6)]
    replicated_layer = kelvin_reading[None]
    caloric_quotient = columns[0] + replicated_layer * (columns[1] + replicated_layer * (columns[2] + replicated_layer * (columns[3] + replicated_layer * columns[4])))
    chemical_heat_content = columns[5] + replicated_layer * (columns[0] + replicated_layer * (columns[1] / 2.0 + replicated_layer * (columns[2] / 3.0 + replicated_layer * (columns[3] / 4.0 + replicated_layer * columns[4] / 5.0))))
    return (caloric_quotient, chemical_heat_content)

def solve_for_kelvin(preserved_vector_lines, nasa_table_weights, component_kind_r_factor):
    prefix_addition_result = preserved_vector_lines[:NS]
    bulk_compactness = lax.optimization_barrier(jnp.sum(prefix_addition_result, axis=0))
    momentum = preserved_vector_lines[NS:NS + 3]
    caloric_content_inner = preserved_vector_lines[NS + 3] - 0.5 * lax.optimization_barrier(jnp.sum(momentum * momentum, axis=0)) / bulk_compactness
    blend_stack_lane = column(component_kind_r_factor, bulk_compactness.ndim)
    kelvin_reading = jnp.ones_like(bulk_compactness)
    for iteration in range(NEWTON):
        caloric_quotient, chemical_heat_content = caloric_fitted_curves_table(nasa_table_weights, kelvin_reading)
        solver_misfit = lax.optimization_barrier(jnp.sum(prefix_addition_result * blend_stack_lane * (chemical_heat_content - kelvin_reading[None]), axis=0)) - caloric_content_inner
        tangent_steepness_fn = lax.optimization_barrier(jnp.sum(prefix_addition_result * blend_stack_lane * (caloric_quotient - 1.0), axis=0))
        kelvin_reading = kelvin_reading - solver_misfit / tangent_steepness_fn
    return kelvin_reading

def nasa_fitted_monomials(preserved_vector_lines, kelvin_reading, nasa_table_weights, component_kind_r_factor):
    prefix_addition_result = preserved_vector_lines[:NS]
    bulk_compactness = lax.optimization_barrier(jnp.sum(prefix_addition_result, axis=0))
    momentum = preserved_vector_lines[NS:NS + 3]
    doubled_norm_motion = lax.optimization_barrier(jnp.sum(momentum * momentum, axis=0)) / (bulk_compactness * bulk_compactness)
    blend_stack_lane = column(component_kind_r_factor, bulk_compactness.ndim)
    caloric_quotient, chemical_heat_content = caloric_fitted_curves_table(nasa_table_weights, kelvin_reading)
    caloric_tiers = blend_stack_lane * (chemical_heat_content - kelvin_reading[None])
    averaged_mixing_law_r = lax.optimization_barrier(jnp.sum(prefix_addition_result * blend_stack_lane, axis=0))
    thrust_load_quiet = averaged_mixing_law_r * kelvin_reading
    heat_quotient_decrement = averaged_mixing_law_r / lax.optimization_barrier(jnp.sum(prefix_addition_result * blend_stack_lane * (caloric_quotient - 1.0), axis=0))
    sound_speed = jnp.sqrt((1.0 + heat_quotient_decrement) * thrust_load_quiet / bulk_compactness)
    force_spatial_jump = blend_stack_lane * kelvin_reading[None] - heat_quotient_decrement[None] * caloric_tiers + 0.5 * heat_quotient_decrement[None] * doubled_norm_motion[None]
    return jnp.concatenate([thrust_load_quiet[None], heat_quotient_decrement[None], sound_speed[None], force_spatial_jump], axis=0)

def reconstruct(values):
    value_zero, value_one, value_two, value_three, value_four = values
    candidate_zero = (2.0 * value_zero - 7.0 * value_one + 11.0 * value_two) / 6.0
    candidate_one = (-value_one + 5.0 * value_two + 2.0 * value_three) / 6.0
    candidate_two = (2.0 * value_two + 5.0 * value_three - value_four) / 6.0
    curve_zero = value_zero - 2.0 * value_one + value_two
    slope_zero = value_zero - 4.0 * value_one + 3.0 * value_two
    curve_one = value_one - 2.0 * value_two + value_three
    slope_one = value_one - value_three
    curve_two = value_two - 2.0 * value_three + value_four
    slope_two = 3.0 * value_two - 4.0 * value_three + value_four
    smooth_zero = 13.0 / 12.0 * curve_zero * curve_zero + 0.25 * slope_zero * slope_zero
    smooth_one = 13.0 / 12.0 * curve_one * curve_one + 0.25 * slope_one * slope_one
    smooth_two = 13.0 / 12.0 * curve_two * curve_two + 0.25 * slope_two * slope_two
    weight_zero = 0.1 / ((EPSILON + smooth_zero) * (EPSILON + smooth_zero))
    weight_one = 0.6 / ((EPSILON + smooth_one) * (EPSILON + smooth_one))
    weight_two = 0.3 / ((EPSILON + smooth_two) * (EPSILON + smooth_two))
    return (weight_zero * candidate_zero + weight_one * candidate_one + weight_two * candidate_two) / (weight_zero + weight_one + weight_two)

def window(array, offset, count, array_axis):
    return lax.slice_in_dim(array, offset, offset + count, axis=array_axis)

def direction_rate(preserved_vector_lines, cell_coef, array_axis, normal, speed):
    cells = preserved_vector_lines.shape[array_axis] - 6
    faces = cells + 1
    bulk_compactness = lax.optimization_barrier(jnp.sum(preserved_vector_lines[:NS], axis=0))
    fractions = preserved_vector_lines[:NS] / bulk_compactness[None]
    velocity = preserved_vector_lines[NS:NS + 3] / bulk_compactness[None]
    passive = preserved_vector_lines[NS + 4:NS + 5] / bulk_compactness[None]
    thrust_load_quiet = cell_coef[0]
    normal_speed = velocity[normal]
    carried = preserved_vector_lines * normal_speed[None]
    flux_rows = [carried[:NS]]
    for component in range(3):
        if component == normal:
            flux_rows.append((carried[NS + component] + thrust_load_quiet)[None])
        else:
            flux_rows.append(carried[NS + component][None])
    flux_rows.append((carried[NS + 3] + thrust_load_quiet * normal_speed)[None])
    flux_rows.append(carried[NS + 4][None])
    physical = jnp.concatenate(flux_rows, axis=0)
    upwind = 0.5 * (physical + speed * preserved_vector_lines)
    downwind = 0.5 * (physical - speed * preserved_vector_lines)

    def average(array):
        return 0.5 * (window(array, 2, faces, array_axis) + window(array, 3, faces, array_axis))
    mean_frac = average(fractions)
    mean_vel = average(velocity)
    mean_passive = average(passive)[0]
    mean_gamma = average(cell_coef[1:2])[0]
    mean_sound = average(cell_coef[2:3])[0]
    mean_slopes = average(cell_coef[3:])
    mean_square = lax.optimization_barrier(jnp.sum(mean_vel * mean_vel, axis=0))
    mean_enthalpy = (mean_sound * mean_sound - lax.optimization_barrier(jnp.sum(mean_frac * mean_slopes, axis=0))) / mean_gamma + mean_square
    inverse = 1.0 / (mean_sound * mean_sound)
    tangents = [component for component in range(3) if component != normal]

    def project(vector):
        total = lax.optimization_barrier(jnp.sum(vector[:NS], axis=0))
        pressure_jump = lax.optimization_barrier(jnp.sum(mean_slopes * vector[:NS], axis=0)) - mean_gamma * lax.optimization_barrier(jnp.sum(mean_vel * vector[NS:NS + 3], axis=0)) + mean_gamma * vector[NS + 3]
        normal_jump = vector[NS + normal] - mean_vel[normal] * total
        scaled = pressure_jump * inverse
        slower = 0.5 * (pressure_jump - mean_sound * normal_jump) * inverse
        faster = 0.5 * (pressure_jump + mean_sound * normal_jump) * inverse
        species = vector[:NS] - mean_frac * scaled[None]
        first_shear = vector[NS + tangents[0]] - mean_vel[tangents[0]] * total
        second_shear = vector[NS + tangents[1]] - mean_vel[tangents[1]] * total
        scalar_wave = vector[NS + 4] - mean_passive * scaled
        return jnp.concatenate([slower[None], species, first_shear[None], second_shear[None], faster[None], scalar_wave[None]], axis=0)
    rising = reconstruct([project(window(upwind, offset, faces, array_axis)) for offset in (0, 1, 2, 3, 4)])
    falling = reconstruct([project(window(downwind, offset, faces, array_axis)) for offset in (5, 4, 3, 2, 1)])
    amplitude = rising + falling
    slower = amplitude[0]
    species = amplitude[1:NS + 1]
    first_shear = amplitude[NS + 1]
    second_shear = amplitude[NS + 2]
    faster = amplitude[NS + 3]
    scalar_wave = amplitude[NS + 4]
    species_total = lax.optimization_barrier(jnp.sum(species, axis=0))
    acoustic = slower + faster
    normal_vel = mean_vel[normal]
    momentum_rows = []
    for component in range(3):
        if component == normal:
            momentum_rows.append((normal_vel - mean_sound) * slower + (normal_vel + mean_sound) * faster + normal_vel * species_total)
        elif component == tangents[0]:
            momentum_rows.append(mean_vel[component] * (acoustic + species_total) + first_shear)
        else:
            momentum_rows.append(mean_vel[component] * (acoustic + species_total) + second_shear)
    energy_row = (mean_enthalpy - normal_vel * mean_sound) * slower + (mean_enthalpy + normal_vel * mean_sound) * faster + lax.optimization_barrier(jnp.sum((mean_square[None] - mean_slopes / mean_gamma[None]) * species, axis=0)) + mean_vel[tangents[0]] * first_shear + mean_vel[tangents[1]] * second_shear
    face_flux = jnp.concatenate([mean_frac * acoustic[None] + species, jnp.stack(momentum_rows, axis=0), energy_row[None], (mean_passive * acoustic + scalar_wave)[None]], axis=0)
    return window(face_flux, 0, cells, array_axis) - window(face_flux, 1, cells, array_axis)

def wall_pad(payload, lower_kind, upper_kind):
    rows_count = payload.shape[0]
    sign_flips = jnp.where(jnp.arange(rows_count) == NS + 2, -1.0, 1.0).astype(payload.dtype).reshape((rows_count, 1, 1, 1))
    lower_copy = jnp.concatenate([payload[..., :1]] * 3, axis=3)
    upper_copy = jnp.concatenate([payload[..., -1:]] * 3, axis=3)
    lower_mirror = payload[..., 2::-1] * sign_flips
    upper_mirror = payload[..., :-4:-1] * sign_flips
    lower_ghost = jnp.where(lower_kind == 1, lower_mirror, lower_copy)
    upper_ghost = jnp.where(upper_kind == 1, upper_mirror, upper_copy)
    return jnp.concatenate([lower_ghost, payload, upper_ghost], axis=3)

def reference(preserved_vector, nasa_table, gas_constant, species_index, face_kind):
    nasa_table_weights = nasa_table[species_index]
    component_kind_r_factor = gas_constant[species_index]
    block_ids = jnp.arange(N_GX, dtype=jnp.int32)

    def cell_block(block_id):
        patch_region = lax.dynamic_slice_in_dim(preserved_vector, (block_id * CX).astype(jnp.int32), CX, 1)
        kelvin_reading = solve_for_kelvin(patch_region, nasa_table_weights, component_kind_r_factor)
        patch_multiplier = nasa_fitted_monomials(patch_region, kelvin_reading, nasa_table_weights, component_kind_r_factor)
        bulk_compactness = lax.optimization_barrier(jnp.sum(patch_region[:NS], axis=0))
        velocity = patch_region[NS:NS + 3] / bulk_compactness[None]
        local_speed = lax.optimization_barrier(jnp.max(jnp.abs(velocity) + patch_multiplier[2][None], axis=(1, 2, 3)))
        return (patch_multiplier, local_speed)
    coef_blocks, speed_blocks = lax.map(cell_block, block_ids)
    cell_coef = jnp.transpose(coef_blocks, (1, 0, 2, 3, 4)).reshape((NS + 3, NX, NY, NZ))
    speeds = lax.optimization_barrier(jnp.max(speed_blocks, axis=0))

    def rate_block(inputs):
        block_id, kinds = inputs
        rows_index = (block_id * CX - 3 + jnp.arange(CX + 6, dtype=jnp.int32)) % NX
        state_x = jnp.take(preserved_vector, rows_index, axis=1)
        coef_x = jnp.take(cell_coef, rows_index, axis=1)
        rate = direction_rate(state_x, coef_x, 1, 0, speeds[0])
        state_mid = state_x[:, 3:3 + CX]
        coef_mid = coef_x[:, 3:3 + CX]
        state_y = jnp.concatenate([state_mid[:, :, -3:], state_mid, state_mid[:, :, :3]], axis=2)
        coef_y = jnp.concatenate([coef_mid[:, :, -3:], coef_mid, coef_mid[:, :, :3]], axis=2)
        rate = rate + direction_rate(state_y, coef_y, 2, 1, speeds[1])
        lower_kind = jnp.repeat(kinds[:, 0], CY).reshape((1, 1, NY, 1))
        upper_kind = jnp.repeat(kinds[:, 1], CY).reshape((1, 1, NY, 1))
        padded_z = wall_pad(jnp.concatenate([state_mid, coef_mid], axis=0), lower_kind, upper_kind)
        rate = rate + direction_rate(padded_z[:NVAR], padded_z[NVAR:], 3, 2, speeds[2])
        return rate
    rate_blocks = lax.map(rate_block, (block_ids, face_kind))
    rate = jnp.transpose(rate_blocks, (1, 0, 2, 3, 4)).reshape((NVAR, NX, NY, NZ))
    return COURANT / jnp.sum(speeds) * rate
```

```python
import functools

import jax
import jax.numpy as jnp
from jax import lax
from jax.experimental import pallas as pl
from jax.experimental.pallas import tpu as pltpu
from jax.sharding import PartitionSpec as P

NS = 9
NVAR = 14
EPSILON = 1e-06
COURANT = 0.8
TOTAL = NVAR
PRIMS = 24
VEL, PASSIVE, GAMMA, SOUND, SLOPES = 9, 12, 13, 14, 15
TABLE = 7 * NS


def fill_table(nasa_ref, gas_ref, index_ref, table_ref):
    for i in range(NS):
        row = index_ref[i]
        gas = gas_ref[row]
        values = [
            gas,
            gas * nasa_ref[row, 5],
            gas * (nasa_ref[row, 0] - 1.0),
            gas * nasa_ref[row, 1] * (1.0 / 2.0),
            gas * nasa_ref[row, 2] * (1.0 / 3.0),
            gas * nasa_ref[row, 3] * (1.0 / 4.0),
            gas * nasa_ref[row, 4] * (1.0 / 5.0),
        ]
        for n, value in enumerate(values):
            table_ref[n * NS + i] = jnp.full(table_ref.shape[1:], value, jnp.float32)


def tree(terms):
    terms = list(terms)
    while len(terms) > 1:
        terms = [a + b for a, b in zip(terms[::2], terms[1::2])] + (
            [terms[-1]] if len(terms) % 2 else []
        )
    return terms[0]


def thermo(u, table_ref):
    rho = tree(u[:NS])
    inverse = 1.0 / rho
    vel = [m * inverse for m in u[NS : NS + 3]]
    square = tree([v * v for v in vel])
    inner = u[NS + 3] - 0.5 * tree([v * m for v, m in zip(vel, u[NS : NS + 3])])
    mix = [tree([u[i] * table_ref[n * NS + i] for i in range(NS)]) for n in range(7)]
    gas, m6, m1, m2, m3, m4, m5 = mix
    c2, c3, c4, c5 = 2.0 * m2, 3.0 * m3, 4.0 * m4, 5.0 * m5
    temp = 1.0 - (tree([m6, m1, m2, m3, m4, m5]) - inner) / tree([m1, c2, c3, c4, c5])

    def heat(t):
        return m1 + t * (c2 + t * (c3 + t * (c4 + t * c5)))

    energy = m6 + temp * (m1 + temp * (m2 + temp * (m3 + temp * (m4 + temp * m5))))
    temp = temp - (energy - inner) / heat(temp)
    pressure = temp * gas
    gamma = gas / heat(temp)
    sound = jnp.sqrt((1.0 + gamma) * pressure * inverse)
    return inverse, vel, square, temp, pressure, gamma, sound


def slopes_of(temp, gamma, square, table_ref):
    kinetic = 0.5 * gamma * square
    result = []
    for i in range(NS):
        k = [table_ref[n * NS + i] for n in range(7)]
        e = k[1] + temp * (k[2] + temp * (k[3] + temp * (k[4] + temp * (k[5] + temp * k[6]))))
        result.append(k[0] * temp - gamma * e + kinetic)
    return result


def reciprocal(x):
    return pl.reciprocal(x, approx=True)


def correction(d):
    d0, d1, d2, d3 = d
    e0, e1, e2 = d1 - d0, d2 - d1, d3 - d2
    h1, h2 = 0.75 * d1, 0.75 * d2
    near, far = h1 * d1 + 0.75 * EPSILON, h2 * d2 + 0.75 * EPSILON
    r0 = reciprocal(e0 * (e0 + h1) + near)
    r1 = reciprocal(e1 * (e1 + h1) + near)
    r2 = reciprocal(e2 * (e2 - h2) + far)
    a = r0 * r0 * (1.0 / 3.0)
    b = r1 * r1
    c = r2 * r2
    g0, g2 = e0 - e1, e1 - e2
    return (a * (g0 + g0) + c * g2) * reciprocal(a + c + (b + b))


def face(normal, up, down, mean, linear, put):
    phi = [mean(SLOPES + i) for i in range(NS)]
    vel = [mean(VEL + i) for i in range(3)]
    gamma, sound = mean(GAMMA), mean(SOUND)
    inv = 1.0 / sound
    inv2, half_inv = inv * inv, 0.5 * inv
    tangents = [t for t in range(3) if t != normal]
    sigma, slow, fast = ([], []), ([], []), ([], [])
    shear = [([], []), ([], [])]
    for side, get in enumerate((up, down)):
        for k in range(4):
            s = get(TOTAL, k)
            m = [get(NS + i, k) for i in range(3)]
            dp = tree([phi[i] * get(i, k) for i in range(NS)]) + gamma * (
                get(NS + 3, k) - tree([vel[i] * m[i] for i in range(3)])
            )
            scaled = dp * inv2
            jump = (m[normal] - vel[normal] * s) * half_inv
            half = 0.5 * scaled
            sigma[side].append(scaled)
            slow[side].append(half - jump)
            fast[side].append(half + jump)
            for n, t in enumerate(tangents):
                shear[n][side].append(m[t] - vel[t] * s)

    def both(pair):
        return correction(pair[0]) - correction(pair[1])

    slower, faster = both(slow), both(fast)
    shears = [both(pair) for pair in shear]
    acoustic = slower + faster
    total, weighted, blend = None, None, None
    for i in range(NS):
        y = mean(i)
        amp = both(
            (
                [up(i, k) - y * sigma[0][k] for k in range(4)],
                [down(i, k) - y * sigma[1][k] for k in range(4)],
            )
        )
        put(i, linear(i) + y * acoustic + amp)
        total = amp if i == 0 else total + amp
        weighted = phi[i] * amp if i == 0 else weighted + phi[i] * amp
        blend = phi[i] * y if i == 0 else blend + phi[i] * y
    z = mean(PASSIVE)
    amp = both(
        (
            [up(NS + 4, k) - z * sigma[0][k] for k in range(4)],
            [down(NS + 4, k) - z * sigma[1][k] for k in range(4)],
        )
    )
    put(NS + 4, linear(NS + 4) + z * acoustic + amp)
    mass = acoustic + total
    swing = sound * (faster - slower)
    put(NS + normal, linear(NS + normal) + vel[normal] * mass + swing)
    for n, t in enumerate(tangents):
        put(NS + t, linear(NS + t) + vel[t] * mass + shears[n])
    square = tree([v * v for v in vel])
    energy = (
        square * mass
        + ((sound * sound - blend) * acoustic - weighted) / gamma
        + vel[normal] * swing
        + vel[tangents[0]] * shears[0]
        + vel[tangents[1]] * shears[1]
    )
    put(NS + 3, linear(NS + 3) + energy)


def fill_cells(u, i, table_ref, prim_ref):
    inverse, vel, square, temp, pressure, gamma, sound = thermo(u, table_ref)
    for k in range(NS):
        prim_ref[k, i] = u[k] * inverse
    for k in range(3):
        prim_ref[VEL + k, i] = vel[k]
    prim_ref[PASSIVE, i] = u[NS + 4] * inverse
    prim_ref[GAMMA, i] = gamma
    prim_ref[SOUND, i] = sound
    for k, value in enumerate(slopes_of(temp, gamma, square, table_ref)):
        prim_ref[SLOPES + k, i] = value
    prim_ref[PRIMS, i] = pressure


def fill_split(u, i, normal, alpha, prim_ref, up_ref, down_ref):
    speed = prim_ref[VEL + normal, i]
    push = 0.5 * prim_ref[PRIMS, i]
    half = 0.5 * speed
    lean = 0.5 * alpha
    plus, minus = half + lean, half - lean
    for ref, factor in ((up_ref, plus), (down_ref, minus)):
        for k in range(NVAR):
            value = u[k] * factor
            if k == NS + normal:
                value = value + push
            if k == NS + 3:
                value = value + push * speed
            ref[k, i] = value
        ref[TOTAL, i] = tree(u[:NS]) * factor


def compute(
    nasa_ref, gas_ref, index_ref, kind_ref, speeds_ref, x_ref, hx_ref, hy_ref, out_ref,
    table_ref, prim_ref, up_ref, down_ref, dup_ref, ddown_ref,
    fx_ref, fz_ref, acc_ref, edge_ref,
):
    lanes = x_ref.shape[1]
    tile = (8, lanes)
    block = 64
    fill_table(nasa_ref, gas_ref, index_ref, table_ref)
    alphas = [speeds_ref[d] for d in range(3)]

    def own(r, x):
        return x_ref[pl.ds(pl.multiple_of(r * block + x * 8, 8), 8), :]

    def turned(r, y):
        return x_ref[pl.ds(r * block + y, 8, stride=8), :]

    def differences(count):
        def step(i, _):
            for k in range(NVAR + 1):
                dup_ref[k, i] = up_ref[k, i + 1] - up_ref[k, i]
                ddown_ref[k, i] = down_ref[k, i + 1] - down_ref[k, i]
            return 0

        lax.fori_loop(0, count, step, 0)

    def faces_across(normal, flux_ref):
        def step(i, _):
            def linear(r):
                here = up_ref[r, i + 2] + down_ref[r, i + 3]
                ahead = dup_ref[r, i + 2] - ddown_ref[r, i + 2]
                return 6.0 * here + (ahead + ahead) + (dup_ref[r, i + 1] - ddown_ref[r, i + 3])

            def put(r, value):
                flux_ref[r, i] = value

            face(
                normal,
                lambda r, k: dup_ref[r, i + k],
                lambda r, k: ddown_ref[r, i + 4 - k],
                lambda q: 0.5 * (prim_ref[q, i + 2] + prim_ref[q, i + 3]),
                linear,
                put,
            )
            return 0

        lax.fori_loop(0, 9, step, 0)

    def y_cells(i, read):
        u = read()
        fill_cells(u, i, table_ref, prim_ref)
        fill_split(u, i, 1, alphas[1], prim_ref, up_ref, down_ref)

    def y_own(y, _):
        y_cells(y + 3, lambda: [turned(r, y) for r in range(NVAR)])
        return 0

    def y_halo(k, _):
        y_cells(k, lambda: [hy_ref[0, r, k] for r in range(NVAR)])
        y_cells(k + 11, lambda: [hy_ref[1, r, k] for r in range(NVAR)])
        return 0

    def x_own(x, _):
        u = [own(r, x) for r in range(NVAR)]
        fill_cells(u, x + 3, table_ref, prim_ref)
        fill_split(u, x + 3, 0, alphas[0], prim_ref, up_ref, down_ref)
        return 0

    def x_halo(k, _):
        for side, base in ((0, 0), (1, 11)):
            u = [hx_ref[side, r, k] for r in range(NVAR)]
            fill_cells(u, k + base, table_ref, prim_ref)
            fill_split(u, k + base, 0, alphas[0], prim_ref, up_ref, down_ref)
        return 0

    lane = lax.broadcasted_iota(jnp.int32, tile, 1)

    width = 16
    spot = lane % width
    reach = spot - 3
    low_wall, high_wall = kind_ref[0] == 1, kind_ref[1] == 1
    low = jnp.where(reach < 0, jnp.where(low_wall, -1 - reach, 0), reach)
    beyond = spot - 13
    high = jnp.where(
        beyond >= 0,
        jnp.where(high_wall, lanes - 1 - beyond, lanes - 1),
        lanes + beyond,
    )
    source = jnp.where(spot < 8, low, high)
    mirrored = ((spot < 3) & low_wall) | ((spot > 12) & high_wall)
    sign = jnp.where(mirrored, -1.0, 1.0)
    group = lane // width

    def gather(values, index):
        return jnp.take_along_axis(values, index, axis=1)

    def z_edge(x, _):
        for r in range(NVAR):
            value = gather(own(r, x), source)
            if r == NS + 2:
                value = value * sign
            edge_ref[r] = jnp.where(group == x, value, edge_ref[r])
        return 0

    def roll(values, shift):
        return values if shift % lanes == 0 else pltpu.roll(values, shift % lanes, 1)

    def z_split(u, i):
        fill_split(u, i, 2, alphas[2], prim_ref, up_ref, down_ref)
        for k in range(NVAR + 1):
            dup_ref[k, i] = roll(up_ref[k, i], -1) - up_ref[k, i]
            ddown_ref[k, i] = roll(down_ref[k, i], -1) - down_ref[k, i]

    def z_own(x, _):
        u = [own(r, x) for r in range(NVAR)]
        z_split(u, x + 3)
        return 0

    def z_faces(x, _):
        i = x + 3

        def linear(r):
            here = up_ref[r, i] + roll(down_ref[r, i], -1)
            ahead = dup_ref[r, i] - ddown_ref[r, i]
            return 6.0 * here + (ahead + ahead) + (
                roll(dup_ref[r, i], 1) - roll(ddown_ref[r, i], -1)
            )

        def mean(q):
            value = prim_ref[q, i]
            return 0.5 * (value + roll(value, -1))

        def put(r, value):
            fz_ref[r, x] = value

        face(
            2,
            lambda r, k: roll(dup_ref[r, i], 2 - k),
            lambda r, k: roll(ddown_ref[r, i], k - 2),
            mean,
            linear,
            put,
        )
        return 0

    lax.fori_loop(0, 3, y_halo, 0)
    lax.fori_loop(0, 8, y_own, 0)
    differences(13)
    faces_across(1, fx_ref)

    def y_rate(y, _):
        for r in range(NVAR):
            acc_ref[pl.ds(r * block + y, 8, stride=8), :] = fx_ref[r, y + 1] - fx_ref[r, y]
        return 0

    lax.fori_loop(0, 8, y_rate, 0)

    lax.fori_loop(0, 3, x_halo, 0)
    lax.fori_loop(0, 8, x_own, 0)
    differences(13)
    faces_across(0, fx_ref)

    for r in range(NVAR):
        edge_ref[r] = jnp.zeros(tile, jnp.float32)
    lax.fori_loop(0, 8, z_edge, 0)
    edge = [edge_ref[r] for r in range(NVAR)]
    fill_cells(edge, 11, table_ref, prim_ref)
    z_split(edge, 11)
    lax.fori_loop(0, 8, z_own, 0)
    lax.fori_loop(0, 9, z_faces, 0)

    scale = (-COURANT / 6.0) / (alphas[0] + alphas[1] + alphas[2])
    near = jnp.where(lane < 2, lane + 3, lane - lanes + 13)
    patched = (lane < 2) | (lane > lanes - 4)

    def finish(x, _):
        first = jnp.clip(width * x + near, 0, lanes - 1)
        below = jnp.full(tile, width * x + 2, jnp.int32)
        for r in range(NVAR):
            edges = fz_ref[r, 8]
            upper = jnp.where(patched, gather(edges, first), fz_ref[r, x])
            lower = jnp.where(lane == 0, gather(edges, below), roll(upper, 1))
            rows = pl.ds(pl.multiple_of(r * block + x * 8, 8), 8)
            rate = (upper - lower) + (fx_ref[r, x + 1] - fx_ref[r, x]) + acc_ref[rows, :]
            out_ref[rows, :] = scale * rate
        return 0

    lax.fori_loop(0, 8, finish, 0)


def increment(nasa_table, gas_constant, species_index, kinds, speeds, flat, hx, hy):
    lanes = flat.shape[1]
    smem = pl.BlockSpec(memory_space=pltpu.SMEM)
    vmem = pl.BlockSpec(memory_space=pltpu.VMEM)

    def buffer(*shape):
        return pltpu.VMEM(shape + (8, lanes), jnp.float32)

    return pl.pallas_call(
        compute,
        out_shape=jax.ShapeDtypeStruct(flat.shape, jnp.float32),
        in_specs=[smem] * 4 + [vmem] * 4,
        out_specs=vmem,
        scratch_shapes=[
            buffer(TABLE),
            buffer(PRIMS + 1, 14),
            buffer(NVAR + 1, 14),
            buffer(NVAR + 1, 14),
            buffer(NVAR + 1, 14),
            buffer(NVAR + 1, 14),
            buffer(NVAR, 9),
            buffer(NVAR, 9),
            pltpu.VMEM(flat.shape, jnp.float32),
            buffer(NVAR),
        ],
        name="increment",
    )(nasa_table, gas_constant, species_index, kinds, speeds, flat, hx, hy)


def speed_kernel(nasa_ref, gas_ref, index_ref, x_ref, out_ref, table_ref):
    block = 64
    fill_table(nasa_ref, gas_ref, index_ref, table_ref)

    def step(x, best):
        u = [x_ref[pl.ds(pl.multiple_of(r * block + x * 8, 8), 8), :] for r in range(NVAR)]
        _, vel, _, _, _, _, sound = thermo(u, table_ref)
        return tuple(jnp.maximum(b, jnp.abs(v) + sound) for b, v in zip(best, vel))

    zero = jnp.zeros((8, x_ref.shape[1]), jnp.float32)
    for d, value in enumerate(lax.fori_loop(0, 8, step, (zero, zero, zero))):
        out_ref[d] = value


def shards(preserved_vector, nasa_table, gas_constant, species_index, face_kind):
    _, nx, ny, lanes = preserved_vector.shape
    flat = preserved_vector.reshape(NVAR * nx * ny, lanes)
    smem = pl.BlockSpec(memory_space=pltpu.SMEM)
    vmem = pl.BlockSpec(memory_space=pltpu.VMEM)
    local = pl.pallas_call(
        speed_kernel,
        out_shape=jax.ShapeDtypeStruct((3, 8, lanes), jnp.float32),
        in_specs=[smem] * 3 + [vmem],
        out_specs=vmem,
        scratch_shapes=[pltpu.VMEM((TABLE, 8, lanes), jnp.float32)],
        name="speeds",
    )(nasa_table, gas_constant, species_index, flat)
    speeds = lax.pmax(jnp.max(local, axis=(1, 2)), ("gx", "gy"))
    speeds = jnp.broadcast_to(speeds[:, None, None], (3, 8, lanes))

    def swap(low, high, axis):
        n = lax.axis_size(axis)
        ahead = [(i, (i + 1) % n) for i in range(n)]
        back = [(b, a) for a, b in ahead]
        return jnp.stack([lax.ppermute(high, axis, ahead), lax.ppermute(low, axis, back)])

    hx = swap(preserved_vector[:, :3], preserved_vector[:, -3:], "gx")
    turned = jnp.swapaxes(preserved_vector, 1, 2)
    hy = swap(turned[:, :3], turned[:, -3:], "gy")
    out = increment(
        nasa_table, gas_constant, species_index, face_kind.reshape(2), speeds, flat, hx, hy
    )
    return out.reshape(preserved_vector.shape)


def solution(mesh):
    return jax.shard_map(
        shards,
        mesh=mesh,
        in_specs=(P(None, "gx", "gy", None), P(), P(), P(), P("gx", "gy", None)),
        out_specs=P(None, "gx", "gy", None),
        check_vma=False,
    )
```

```python
import functools

import jax
import jax.numpy as jnp
from jax import lax
from jax.experimental import pallas as pl
from jax.experimental.pallas import tpu as pltpu
from jax.sharding import PartitionSpec as P

NS = 9
NVAR = 14
EPSILON = 1e-06
COURANT = 0.8
TOTAL = NVAR
PRIMS = 24
VEL, PASSIVE, GAMMA, SOUND, SLOPES = 9, 12, 13, 14, 15
TABLE = 7 * NS


def fill_table(nasa_ref, gas_ref, index_ref, table_ref):
    for i in range(NS):
        row = index_ref[i]
        gas = gas_ref[row]
        values = [
            gas,
            gas * nasa_ref[5, row],
            gas * (nasa_ref[0, row] - 1.0),
            gas * nasa_ref[1, row] * (1.0 / 2.0),
            gas * nasa_ref[2, row] * (1.0 / 3.0),
            gas * nasa_ref[3, row] * (1.0 / 4.0),
            gas * nasa_ref[4, row] * (1.0 / 5.0),
        ]
        for n, value in enumerate(values):
            table_ref[n * NS + i] = jnp.full(table_ref.shape[1:], value, jnp.float32)


def tree(terms):
    terms = list(terms)
    while len(terms) > 1:
        terms = [a + b for a, b in zip(terms[::2], terms[1::2])] + (
            [terms[-1]] if len(terms) % 2 else []
        )
    return terms[0]


def thermo(u, table_ref):
    rho = tree(u[:NS])
    inverse = 1.0 / rho
    vel = [m * inverse for m in u[NS : NS + 3]]
    square = tree([v * v for v in vel])
    inner = u[NS + 3] - 0.5 * tree([v * m for v, m in zip(vel, u[NS : NS + 3])])
    mix = [tree([u[i] * table_ref[n * NS + i] for i in range(NS)]) for n in range(7)]
    gas, m6, m1, m2, m3, m4, m5 = mix
    c2, c3, c4, c5 = 2.0 * m2, 3.0 * m3, 4.0 * m4, 5.0 * m5
    temp = 1.0 - (tree([m6, m1, m2, m3, m4, m5]) - inner) / tree([m1, c2, c3, c4, c5])

    def heat(t):
        return m1 + t * (c2 + t * (c3 + t * (c4 + t * c5)))

    energy = m6 + temp * (m1 + temp * (m2 + temp * (m3 + temp * (m4 + temp * m5))))
    temp = temp - (energy - inner) / heat(temp)
    pressure = temp * gas
    gamma = gas / heat(temp)
    sound = jnp.sqrt((1.0 + gamma) * pressure * inverse)
    return inverse, vel, square, temp, pressure, gamma, sound


def slopes_of(temp, gamma, square, table_ref):
    kinetic = 0.5 * gamma * square
    result = []
    for i in range(NS):
        k = [table_ref[n * NS + i] for n in range(7)]
        e = k[1] + temp * (k[2] + temp * (k[3] + temp * (k[4] + temp * (k[5] + temp * k[6]))))
        result.append(k[0] * temp - gamma * e + kinetic)
    return result


def reciprocal(x):
    return pl.reciprocal(x, approx=True)


def correction(d):
    d0, d1, d2, d3 = d
    e0, e1, e2 = d1 - d0, d2 - d1, d3 - d2
    h1, h2 = 0.75 * d1, 0.75 * d2
    near, far = h1 * d1 + 0.75 * EPSILON, h2 * d2 + 0.75 * EPSILON
    r0 = reciprocal(e0 * (e0 + h1) + near)
    r1 = reciprocal(e1 * (e1 + h1) + near)
    r2 = reciprocal(e2 * (e2 - h2) + far)
    a = r0 * r0 * (1.0 / 3.0)
    b = r1 * r1
    c = r2 * r2
    g0, g2 = e0 - e1, e1 - e2
    return (a * (g0 + g0) + c * g2) * reciprocal(a + c + (b + b))


def face(normal, up, down, mean, linear, put):
    phi = [mean(SLOPES + i) for i in range(NS)]
    vel = [mean(VEL + i) for i in range(3)]
    gamma, sound = mean(GAMMA), mean(SOUND)
    inv = 1.0 / sound
    inv2, half_inv = inv * inv, 0.5 * inv
    tangents = [t for t in range(3) if t != normal]
    sigma, slow, fast = ([], []), ([], []), ([], [])
    shear = [([], []), ([], [])]
    for side, get in enumerate((up, down)):
        for k in range(4):
            s = get(TOTAL, k)
            m = [get(NS + i, k) for i in range(3)]
            dp = tree([phi[i] * get(i, k) for i in range(NS)]) + gamma * (
                get(NS + 3, k) - tree([vel[i] * m[i] for i in range(3)])
            )
            scaled = dp * inv2
            jump = (m[normal] - vel[normal] * s) * half_inv
            half = 0.5 * scaled
            sigma[side].append(scaled)
            slow[side].append(half - jump)
            fast[side].append(half + jump)
            for n, t in enumerate(tangents):
                shear[n][side].append(m[t] - vel[t] * s)

    def both(pair):
        return correction(pair[0]) - correction(pair[1])

    slower, faster = both(slow), both(fast)
    shears = [both(pair) for pair in shear]
    acoustic = slower + faster
    total, weighted, blend = None, None, None
    for i in range(NS):
        y = mean(i)
        amp = both(
            (
                [up(i, k) - y * sigma[0][k] for k in range(4)],
                [down(i, k) - y * sigma[1][k] for k in range(4)],
            )
        )
        put(i, linear(i) + y * acoustic + amp)
        total = amp if i == 0 else total + amp
        weighted = phi[i] * amp if i == 0 else weighted + phi[i] * amp
        blend = phi[i] * y if i == 0 else blend + phi[i] * y
    z = mean(PASSIVE)
    amp = both(
        (
            [up(NS + 4, k) - z * sigma[0][k] for k in range(4)],
            [down(NS + 4, k) - z * sigma[1][k] for k in range(4)],
        )
    )
    put(NS + 4, linear(NS + 4) + z * acoustic + amp)
    mass = acoustic + total
    swing = sound * (faster - slower)
    put(NS + normal, linear(NS + normal) + vel[normal] * mass + swing)
    for n, t in enumerate(tangents):
        put(NS + t, linear(NS + t) + vel[t] * mass + shears[n])
    square = tree([v * v for v in vel])
    energy = (
        square * mass
        + ((sound * sound - blend) * acoustic - weighted) / gamma
        + vel[normal] * swing
        + vel[tangents[0]] * shears[0]
        + vel[tangents[1]] * shears[1]
    )
    put(NS + 3, linear(NS + 3) + energy)


def fill_cells(u, i, table_ref, prim_ref):
    inverse, vel, square, temp, pressure, gamma, sound = thermo(u, table_ref)
    for k in range(NS):
        prim_ref[k, i] = u[k] * inverse
    for k in range(3):
        prim_ref[VEL + k, i] = vel[k]
    prim_ref[PASSIVE, i] = u[NS + 4] * inverse
    prim_ref[GAMMA, i] = gamma
    prim_ref[SOUND, i] = sound
    for k, value in enumerate(slopes_of(temp, gamma, square, table_ref)):
        prim_ref[SLOPES + k, i] = value
    prim_ref[PRIMS, i] = pressure


def fill_split(u, i, normal, alpha, prim_ref, up_ref, down_ref):
    speed = prim_ref[VEL + normal, i]
    push = 0.5 * prim_ref[PRIMS, i]
    half = 0.5 * speed
    lean = 0.5 * alpha
    plus, minus = half + lean, half - lean
    for ref, factor in ((up_ref, plus), (down_ref, minus)):
        for k in range(NVAR):
            value = u[k] * factor
            if k == NS + normal:
                value = value + push
            if k == NS + 3:
                value = value + push * speed
            ref[k, i] = value
        ref[TOTAL, i] = tree(u[:NS]) * factor


def compute(
    nasa_ref, gas_ref, index_ref, kind_ref, speeds_ref, x_ref, hx_ref, hy_ref, out_ref,
    table_ref, prim_ref, up_ref, down_ref, dup_ref, ddown_ref,
    fx_ref, fz_ref, acc_ref, edge_ref,
):
    lanes = x_ref.shape[1]
    tile = (8, lanes)
    block = 64
    fill_table(nasa_ref, gas_ref, index_ref, table_ref)
    alphas = [speeds_ref[d] for d in range(3)]

    def own(r, x):
        return x_ref[pl.ds(pl.multiple_of(r * block + x * 8, 8), 8), :]

    def turned(r, y):
        return x_ref[pl.ds(r * block + y, 8, stride=8), :]

    def differences(count):
        def step(i, _):
            for k in range(NVAR + 1):
                dup_ref[k, i] = up_ref[k, i + 1] - up_ref[k, i]
                ddown_ref[k, i] = down_ref[k, i + 1] - down_ref[k, i]
            return 0

        lax.fori_loop(0, count, step, 0)

    def faces_across(normal, flux_ref):
        def step(i, _):
            def linear(r):
                here = up_ref[r, i + 2] + down_ref[r, i + 3]
                ahead = dup_ref[r, i + 2] - ddown_ref[r, i + 2]
                return 6.0 * here + (ahead + ahead) + (dup_ref[r, i + 1] - ddown_ref[r, i + 3])

            def put(r, value):
                flux_ref[r, i] = value

            face(
                normal,
                lambda r, k: dup_ref[r, i + k],
                lambda r, k: ddown_ref[r, i + 4 - k],
                lambda q: 0.5 * (prim_ref[q, i + 2] + prim_ref[q, i + 3]),
                linear,
                put,
            )
            return 0

        lax.fori_loop(0, 9, step, 0)

    def y_cells(i, read):
        u = read()
        fill_cells(u, i, table_ref, prim_ref)
        fill_split(u, i, 1, alphas[1], prim_ref, up_ref, down_ref)

    def y_own(y, _):
        y_cells(y + 3, lambda: [turned(r, y) for r in range(NVAR)])
        return 0

    def y_halo(k, _):
        for side, base in ((0, 0), (1, 11)):
            first = side * NVAR * 24 + k
            y_cells(
                k + base,
                lambda: [hy_ref[pl.ds(first + r * 24, 8, stride=3), :] for r in range(NVAR)],
            )
        return 0

    def x_own(x, _):
        u = [own(r, x) for r in range(NVAR)]
        fill_cells(u, x + 3, table_ref, prim_ref)
        fill_split(u, x + 3, 0, alphas[0], prim_ref, up_ref, down_ref)
        return 0

    def x_halo(k, _):
        for side, base in ((0, 0), (1, 11)):
            u = [hx_ref[side, r, k] for r in range(NVAR)]
            fill_cells(u, k + base, table_ref, prim_ref)
            fill_split(u, k + base, 0, alphas[0], prim_ref, up_ref, down_ref)
        return 0

    lane = lax.broadcasted_iota(jnp.int32, tile, 1)

    width = 16
    spot = lane % width
    reach = spot - 3
    low_wall, high_wall = kind_ref[0] == 1, kind_ref[1] == 1
    low = jnp.where(reach < 0, jnp.where(low_wall, -1 - reach, 0), reach)
    beyond = spot - 13
    high = jnp.where(
        beyond >= 0,
        jnp.where(high_wall, lanes - 1 - beyond, lanes - 1),
        lanes + beyond,
    )
    source = jnp.where(spot < 8, low, high)
    mirrored = ((spot < 3) & low_wall) | ((spot > 12) & high_wall)
    sign = jnp.where(mirrored, -1.0, 1.0)
    group = lane // width

    def gather(values, index):
        return jnp.take_along_axis(values, index, axis=1)

    def z_edge(x, _):
        for r in range(NVAR):
            value = gather(own(r, x), source)
            if r == NS + 2:
                value = value * sign
            edge_ref[r] = jnp.where(group == x, value, edge_ref[r])
        return 0

    def roll(values, shift):
        return values if shift % lanes == 0 else pltpu.roll(values, shift % lanes, 1)

    def z_split(u, i):
        fill_split(u, i, 2, alphas[2], prim_ref, up_ref, down_ref)
        for k in range(NVAR + 1):
            dup_ref[k, i] = roll(up_ref[k, i], -1) - up_ref[k, i]
            ddown_ref[k, i] = roll(down_ref[k, i], -1) - down_ref[k, i]

    def z_own(x, _):
        u = [own(r, x) for r in range(NVAR)]
        z_split(u, x + 3)
        return 0

    def z_faces(x, _):
        i = x + 3

        def linear(r):
            here = up_ref[r, i] + roll(down_ref[r, i], -1)
            ahead = dup_ref[r, i] - ddown_ref[r, i]
            return 6.0 * here + (ahead + ahead) + (
                roll(dup_ref[r, i], 1) - roll(ddown_ref[r, i], -1)
            )

        def mean(q):
            value = prim_ref[q, i]
            return 0.5 * (value + roll(value, -1))

        def put(r, value):
            fz_ref[r, x] = value

        face(
            2,
            lambda r, k: roll(dup_ref[r, i], 2 - k),
            lambda r, k: roll(ddown_ref[r, i], k - 2),
            mean,
            linear,
            put,
        )
        return 0

    lax.fori_loop(0, 3, y_halo, 0)
    lax.fori_loop(0, 8, y_own, 0)
    differences(13)
    faces_across(1, fx_ref)

    def y_rate(y, _):
        for r in range(NVAR):
            acc_ref[pl.ds(r * block + y, 8, stride=8), :] = fx_ref[r, y + 1] - fx_ref[r, y]
        return 0

    lax.fori_loop(0, 8, y_rate, 0)

    lax.fori_loop(0, 3, x_halo, 0)
    lax.fori_loop(0, 8, x_own, 0)
    differences(13)
    faces_across(0, fx_ref)

    for r in range(NVAR):
        edge_ref[r] = jnp.zeros(tile, jnp.float32)
    lax.fori_loop(0, 8, z_edge, 0)
    edge = [edge_ref[r] for r in range(NVAR)]
    fill_cells(edge, 11, table_ref, prim_ref)
    z_split(edge, 11)
    lax.fori_loop(0, 8, z_own, 0)
    lax.fori_loop(0, 9, z_faces, 0)

    scale = (-COURANT / 6.0) / (alphas[0] + alphas[1] + alphas[2])
    near = jnp.where(lane < 2, lane + 3, lane - lanes + 13)
    patched = (lane < 2) | (lane > lanes - 4)

    def finish(x, _):
        first = jnp.clip(width * x + near, 0, lanes - 1)
        below = jnp.full(tile, width * x + 2, jnp.int32)
        for r in range(NVAR):
            edges = fz_ref[r, 8]
            upper = jnp.where(patched, gather(edges, first), fz_ref[r, x])
            lower = jnp.where(lane == 0, gather(edges, below), roll(upper, 1))
            rows = pl.ds(pl.multiple_of(r * block + x * 8, 8), 8)
            rate = (upper - lower) + (fx_ref[r, x + 1] - fx_ref[r, x]) + acc_ref[rows, :]
            out_ref[rows, :] = scale * rate
        return 0

    lax.fori_loop(0, 8, finish, 0)


def increment(nasa_table, gas_constant, species_index, kinds, speeds, flat, hx, hy):
    lanes = flat.shape[1]
    smem = pl.BlockSpec(memory_space=pltpu.SMEM)
    vmem = pl.BlockSpec(memory_space=pltpu.VMEM)

    def buffer(*shape):
        return pltpu.VMEM(shape + (8, lanes), jnp.float32)

    return pl.pallas_call(
        compute,
        out_shape=jax.ShapeDtypeStruct(flat.shape, jnp.float32),
        in_specs=[smem] * 4 + [vmem] * 4,
        out_specs=vmem,
        scratch_shapes=[
            buffer(TABLE),
            buffer(PRIMS + 1, 14),
            buffer(NVAR + 1, 14),
            buffer(NVAR + 1, 14),
            buffer(NVAR + 1, 14),
            buffer(NVAR + 1, 14),
            buffer(NVAR, 9),
            buffer(NVAR, 9),
            pltpu.VMEM(flat.shape, jnp.float32),
            buffer(NVAR),
        ],
        name="increment",
    )(nasa_table, gas_constant, species_index, kinds, speeds, flat, hx, hy)


MESH = pl.DeviceIdType.MESH


def exchange(
    size_x, size_y,
    nasa_ref, gas_ref, index_ref, x_ref, source_ref,
    speeds_ref, hx_ref, hy_ref,
    table_ref, mine_ref, line_ref, slots_y, slots_x,
    small_send, recv_y, recv_x, big_send, big_recv,
):
    gx, gy = lax.axis_index("gx"), lax.axis_index("gy")
    nx, ny = source_ref.shape[1], source_ref.shape[2]

    def along_x(offset):
        return (lax.rem(gx + offset, size_x), gy)

    def along_y(offset):
        return (gx, lax.rem(gy + offset, size_y))

    barrier = pltpu.get_barrier_semaphore()
    for n, along in ((size_x, along_x), (size_y, along_y)):
        for offset in range(1, n):
            pl.semaphore_signal(barrier, inc=1, device_id=along(offset), device_id_type=MESH)
    pl.semaphore_wait(barrier, size_x + size_y - 2)

    halos = []
    for n, (source, target, device) in enumerate(
        (
            (source_ref.at[:, pl.ds(nx - 3, 3)], hx_ref.at[0], along_x(1)),
            (source_ref.at[:, pl.ds(0, 3)], hx_ref.at[1], along_x(size_x - 1)),
            (source_ref.at[:, :, pl.ds(ny - 3, 3)], hy_ref.at[0], along_y(1)),
            (source_ref.at[:, :, pl.ds(0, 3)], hy_ref.at[1], along_y(size_y - 1)),
        )
    ):
        copy = pltpu.make_async_remote_copy(
            src_ref=source,
            dst_ref=target,
            send_sem=big_send.at[n],
            recv_sem=big_recv.at[n],
            device_id=device,
            device_id_type=MESH,
        )
        copy.start()
        halos.append(copy)

    fill_table(nasa_ref, gas_ref, index_ref, table_ref)
    block = nx * ny

    def step(x, best):
        u = [x_ref[pl.ds(pl.multiple_of(r * block + x * 8, 8), 8), :] for r in range(NVAR)]
        _, vel, _, _, _, _, sound = thermo(u, table_ref)
        return tuple(jnp.maximum(b, jnp.abs(v) + sound) for b, v in zip(best, vel))

    tile = mine_ref.shape
    zero = jnp.zeros(tile, jnp.float32)
    best = lax.fori_loop(0, nx, step, (zero, zero, zero))
    best = [jnp.max(b, axis=(0, 1), keepdims=True) for b in best]
    row = lax.broadcasted_iota(jnp.int32, tile, 0)
    value = jnp.where(row == 0, best[0], jnp.where(row == 1, best[1], best[2]))

    for n, along, held, slots, recv, base in (
        (size_y, along_y, mine_ref, slots_y, recv_y, 0),
        (size_x, along_x, line_ref, slots_x, recv_x, size_y),
    ):
        held[...] = value
        copies = []
        for offset in range(1, n):
            copy = pltpu.make_async_remote_copy(
                src_ref=held,
                dst_ref=slots.at[offset],
                send_sem=small_send.at[base + offset],
                recv_sem=recv.at[offset],
                device_id=along(offset),
                device_id_type=MESH,
            )
            copy.start()
            copies.append(copy)
        for offset, copy in enumerate(copies, 1):
            copy.wait()
            value = jnp.maximum(value, slots[offset])
    for d in range(3):
        speeds_ref[d] = jnp.broadcast_to(value[d : d + 1], tile)
    for copy in halos:
        copy.wait()


def shards(preserved_vector, nasa_table, gas_constant, species_index, face_kind):
    _, nx, ny, lanes = preserved_vector.shape
    size_x, size_y = lax.axis_size("gx"), lax.axis_size("gy")
    flat = preserved_vector.reshape(NVAR * nx * ny, lanes)
    nasa_table = nasa_table.T
    smem = pl.BlockSpec(memory_space=pltpu.SMEM)
    vmem = pl.BlockSpec(memory_space=pltpu.VMEM)
    anywhere = pl.BlockSpec(memory_space=pl.ANY)
    shape = functools.partial(jax.ShapeDtypeStruct, dtype=jnp.float32)
    dma = pltpu.SemaphoreType.DMA
    speeds, hx, hy = pl.pallas_call(
        functools.partial(exchange, size_x, size_y),
        out_shape=(
            shape((3, 8, lanes)),
            shape((2, NVAR, 3, ny, 1, lanes)),
            shape((2, NVAR, nx, 3, 1, lanes)),
        ),
        in_specs=[smem] * 3 + [vmem, anywhere],
        out_specs=(vmem, anywhere, anywhere),
        scratch_shapes=[
            pltpu.VMEM((TABLE, 8, lanes), jnp.float32),
            pltpu.VMEM((8, lanes), jnp.float32),
            pltpu.VMEM((8, lanes), jnp.float32),
            pltpu.VMEM((size_y, 8, lanes), jnp.float32),
            pltpu.VMEM((size_x, 8, lanes), jnp.float32),
            dma((size_x + size_y,)),
            dma((size_y,)),
            dma((size_x,)),
            dma((4,)),
            dma((4,)),
        ],
        compiler_params=pltpu.CompilerParams(collective_id=0, has_side_effects=True),
        name="exchange",
    )(
        nasa_table, gas_constant, species_index, flat,
        preserved_vector.reshape(NVAR, nx, ny, 1, lanes),
    )
    out = increment(
        nasa_table, gas_constant, species_index, face_kind.reshape(2), speeds, flat,
        hx.reshape(2, NVAR, 3, ny, lanes), hy.reshape(2 * NVAR * nx * 3, lanes),
    )
    return out.reshape(preserved_vector.shape)


def solution(mesh):
    return jax.shard_map(
        shards,
        mesh=mesh,
        in_specs=(P(None, "gx", "gy", None), P(), P(), P(), P("gx", "gy", None)),
        out_specs=P(None, "gx", "gy", None),
        check_vma=False,
    )
```

```python
import functools

import jax
import jax.numpy as jnp
from jax import lax
from jax.experimental import pallas as pl
from jax.experimental.pallas import tpu as pltpu
from jax.sharding import PartitionSpec as P

NS = 9
NVAR = 14
EPSILON = 1e-06
COURANT = 0.8
TOTAL = NVAR
PRIMS = 24
VEL, PASSIVE, GAMMA, SOUND, SLOPES = 9, 12, 13, 14, 15
TABLE = 7 * NS


def fill_table(nasa_ref, gas_ref, index_ref, table_ref):
    for i in range(NS):
        row = index_ref[i]
        gas = gas_ref[row]
        values = [
            gas,
            gas * nasa_ref[5, row],
            gas * (nasa_ref[0, row] - 1.0),
            gas * nasa_ref[1, row] * (1.0 / 2.0),
            gas * nasa_ref[2, row] * (1.0 / 3.0),
            gas * nasa_ref[3, row] * (1.0 / 4.0),
            gas * nasa_ref[4, row] * (1.0 / 5.0),
        ]
        for n, value in enumerate(values):
            table_ref[n * NS + i] = jnp.full(table_ref.shape[1:], value, jnp.float32)


def tree(terms):
    terms = list(terms)
    while len(terms) > 1:
        terms = [a + b for a, b in zip(terms[::2], terms[1::2])] + (
            [terms[-1]] if len(terms) % 2 else []
        )
    return terms[0]


def thermo(u, table_ref):
    rho = tree(u[:NS])
    inverse = 1.0 / rho
    vel = [m * inverse for m in u[NS : NS + 3]]
    square = tree([v * v for v in vel])
    inner = u[NS + 3] - 0.5 * tree([v * m for v, m in zip(vel, u[NS : NS + 3])])
    mix = [tree([u[i] * table_ref[n * NS + i] for i in range(NS)]) for n in range(7)]
    gas, m6, m1, m2, m3, m4, m5 = mix
    c2, c3, c4, c5 = 2.0 * m2, 3.0 * m3, 4.0 * m4, 5.0 * m5
    temp = 1.0 - (tree([m6, m1, m2, m3, m4, m5]) - inner) / tree([m1, c2, c3, c4, c5])

    def heat(t):
        return m1 + t * (c2 + t * (c3 + t * (c4 + t * c5)))

    energy = m6 + temp * (m1 + temp * (m2 + temp * (m3 + temp * (m4 + temp * m5))))
    temp = temp - (energy - inner) / heat(temp)
    pressure = temp * gas
    gamma = gas / heat(temp)
    sound = jnp.sqrt((1.0 + gamma) * pressure * inverse)
    return inverse, vel, square, temp, pressure, gamma, sound


def slopes_of(temp, gamma, square, table_ref):
    kinetic = 0.5 * gamma * square
    result = []
    for i in range(NS):
        k = [table_ref[n * NS + i] for n in range(7)]
        e = k[1] + temp * (k[2] + temp * (k[3] + temp * (k[4] + temp * (k[5] + temp * k[6]))))
        result.append(k[0] * temp - gamma * e + kinetic)
    return result


def reciprocal(x):
    return pl.reciprocal(x, approx=True)


def correction(d):
    d0, d1, d2, d3 = d
    e0, e1, e2 = d1 - d0, d2 - d1, d3 - d2
    h1, h2 = 0.75 * d1, 0.75 * d2
    near, far = h1 * d1 + 0.75 * EPSILON, h2 * d2 + 0.75 * EPSILON
    r0 = reciprocal(e0 * (e0 + h1) + near)
    r1 = reciprocal(e1 * (e1 + h1) + near)
    r2 = reciprocal(e2 * (e2 - h2) + far)
    a = r0 * r0 * (1.0 / 3.0)
    b = r1 * r1
    c = r2 * r2
    g0, g2 = e0 - e1, e1 - e2
    return (a * (g0 + g0) + c * g2) * reciprocal(a + c + (b + b))


def face(normal, up, down, mean, linear, put):
    phi = [mean(SLOPES + i) for i in range(NS)]
    vel = [mean(VEL + i) for i in range(3)]
    gamma, sound = mean(GAMMA), mean(SOUND)
    inv = 1.0 / sound
    inv2, half_inv = inv * inv, 0.5 * inv
    tangents = [t for t in range(3) if t != normal]
    sigma, slow, fast = ([], []), ([], []), ([], [])
    shear = [([], []), ([], [])]
    for side, get in enumerate((up, down)):
        for k in range(4):
            s = get(TOTAL, k)
            m = [get(NS + i, k) for i in range(3)]
            dp = tree([phi[i] * get(i, k) for i in range(NS)]) + gamma * (
                get(NS + 3, k) - tree([vel[i] * m[i] for i in range(3)])
            )
            scaled = dp * inv2
            jump = (m[normal] - vel[normal] * s) * half_inv
            half = 0.5 * scaled
            sigma[side].append(scaled)
            slow[side].append(half - jump)
            fast[side].append(half + jump)
            for n, t in enumerate(tangents):
                shear[n][side].append(m[t] - vel[t] * s)

    def both(pair):
        return correction(pair[0]) - correction(pair[1])

    slower, faster = both(slow), both(fast)
    shears = [both(pair) for pair in shear]
    acoustic = slower + faster
    total, weighted, blend = None, None, None
    for i in range(NS):
        y = mean(i)
        amp = both(
            (
                [up(i, k) - y * sigma[0][k] for k in range(4)],
                [down(i, k) - y * sigma[1][k] for k in range(4)],
            )
        )
        put(i, linear(i) + y * acoustic + amp)
        total = amp if i == 0 else total + amp
        weighted = phi[i] * amp if i == 0 else weighted + phi[i] * amp
        blend = phi[i] * y if i == 0 else blend + phi[i] * y
    z = mean(PASSIVE)
    amp = both(
        (
            [up(NS + 4, k) - z * sigma[0][k] for k in range(4)],
            [down(NS + 4, k) - z * sigma[1][k] for k in range(4)],
        )
    )
    put(NS + 4, linear(NS + 4) + z * acoustic + amp)
    mass = acoustic + total
    swing = sound * (faster - slower)
    put(NS + normal, linear(NS + normal) + vel[normal] * mass + swing)
    for n, t in enumerate(tangents):
        put(NS + t, linear(NS + t) + vel[t] * mass + shears[n])
    square = tree([v * v for v in vel])
    energy = (
        square * mass
        + ((sound * sound - blend) * acoustic - weighted) / gamma
        + vel[normal] * swing
        + vel[tangents[0]] * shears[0]
        + vel[tangents[1]] * shears[1]
    )
    put(NS + 3, linear(NS + 3) + energy)


def fill_cells(u, i, table_ref, prim_ref):
    inverse, vel, square, temp, pressure, gamma, sound = thermo(u, table_ref)
    for k in range(NS):
        prim_ref[k, i] = u[k] * inverse
    for k in range(3):
        prim_ref[VEL + k, i] = vel[k]
    prim_ref[PASSIVE, i] = u[NS + 4] * inverse
    prim_ref[GAMMA, i] = gamma
    prim_ref[SOUND, i] = sound
    for k, value in enumerate(slopes_of(temp, gamma, square, table_ref)):
        prim_ref[SLOPES + k, i] = value
    prim_ref[PRIMS, i] = pressure


def fill_split(u, i, normal, alpha, prim_ref, up_ref, down_ref):
    speed = prim_ref[VEL + normal, i]
    push = 0.5 * prim_ref[PRIMS, i]
    half = 0.5 * speed
    lean = 0.5 * alpha
    plus, minus = half + lean, half - lean
    for ref, factor in ((up_ref, plus), (down_ref, minus)):
        for k in range(NVAR):
            value = u[k] * factor
            if k == NS + normal:
                value = value + push
            if k == NS + 3:
                value = value + push * speed
            ref[k, i] = value
        ref[TOTAL, i] = tree(u[:NS]) * factor


MESH = pl.DeviceIdType.MESH


def fused(
    size_x, size_y,
    nasa_ref, gas_ref, index_ref, kind_ref, flat_ref, planes_ref, source_ref, out_ref,
    x_ref, hx_ref, hy_ref, mine_ref, line_ref, slots_y, slots_x,
    table_ref, prim_ref, turn_ref, up_ref, down_ref, dup_ref, ddown_ref,
    fx_ref, fz_ref, acc_ref, edge_ref,
    load_sem, small_send, recv_y, recv_x, big_send, big_recv,
):
    load = pltpu.make_async_copy(flat_ref, x_ref, load_sem)
    load.start()
    gx, gy = lax.axis_index("gx"), lax.axis_index("gy")
    nx, ny = planes_ref.shape[1], planes_ref.shape[2]

    def along_x(offset):
        return (lax.rem(gx + offset, size_x), gy)

    def along_y(offset):
        return (gx, lax.rem(gy + offset, size_y))

    barrier = pltpu.get_barrier_semaphore()
    for n, along in ((size_x, along_x), (size_y, along_y)):
        for offset in range(1, n):
            pl.semaphore_signal(barrier, inc=1, device_id=along(offset), device_id_type=MESH)
    fill_table(nasa_ref, gas_ref, index_ref, table_ref)
    pl.semaphore_wait(barrier, size_x + size_y - 2)

    halos = []
    for n, (source, target, device) in enumerate(
        (
            (planes_ref.at[:, pl.ds(nx - 3, 3)], hx_ref.at[0], along_x(1)),
            (planes_ref.at[:, pl.ds(0, 3)], hx_ref.at[1], along_x(size_x - 1)),
            (source_ref.at[:, :, pl.ds(ny - 3, 3)], hy_ref.at[0], along_y(1)),
            (source_ref.at[:, :, pl.ds(0, 3)], hy_ref.at[1], along_y(size_y - 1)),
        )
    ):
        copy = pltpu.make_async_remote_copy(
            src_ref=source,
            dst_ref=target,
            send_sem=big_send.at[n],
            recv_sem=big_recv.at[n],
            device_id=device,
            device_id_type=MESH,
        )
        copy.start()
        halos.append(copy)
    load.wait()

    lanes = x_ref.shape[1]
    tile = (8, lanes)
    block = nx * ny

    def own(r, x):
        return x_ref[pl.ds(pl.multiple_of(r * block + x * 8, 8), 8), :]

    def turned(r, y):
        return x_ref[pl.ds(r * block + y, 8, stride=8), :]

    def differences(count):
        def step(i, _):
            for k in range(NVAR + 1):
                dup_ref[k, i] = up_ref[k, i + 1] - up_ref[k, i]
                ddown_ref[k, i] = down_ref[k, i + 1] - down_ref[k, i]
            return 0

        lax.fori_loop(0, count, step, 0)

    def faces_across(normal, prim_ref, flux_ref):
        def step(i, _):
            def linear(r):
                here = up_ref[r, i + 2] + down_ref[r, i + 3]
                ahead = dup_ref[r, i + 2] - ddown_ref[r, i + 2]
                return 6.0 * here + (ahead + ahead) + (dup_ref[r, i + 1] - ddown_ref[r, i + 3])

            def put(r, value):
                flux_ref[r, i] = value

            face(
                normal,
                lambda r, k: dup_ref[r, i + k],
                lambda r, k: ddown_ref[r, i + 4 - k],
                lambda q: 0.5 * (prim_ref[q, i + 2] + prim_ref[q, i + 3]),
                linear,
                put,
            )
            return 0

        lax.fori_loop(0, 9, step, 0)

    def y_halo_tile(side, r, k):
        return hy_ref[side, r, :, k, 0, :]

    def cells_halo(normal, prims, read):
        def step(k, _):
            for side, base in ((0, 0), (1, 11)):
                u = [read(side, r, k) for r in range(NVAR)]
                fill_cells(u, k + base, table_ref, prims)
                fill_split(u, k + base, normal, alphas[normal], prims, up_ref, down_ref)
            return 0

        lax.fori_loop(0, 3, step, 0)

    def split_own(normal, prims, read):
        def step(n, _):
            u = [read(r, n) for r in range(NVAR)]
            fill_split(u, n + 3, normal, alphas[normal], prims, up_ref, down_ref)
            return 0

        lax.fori_loop(0, 8, step, 0)

    def y_prims(y, _):
        fill_cells([turned(r, y) for r in range(NVAR)], y + 3, table_ref, turn_ref)
        return 0

    lane = lax.broadcasted_iota(jnp.int32, tile, 1)

    width = 16
    spot = lane % width
    reach = spot - 3
    low_wall, high_wall = kind_ref[0] == 1, kind_ref[1] == 1
    low = jnp.where(reach < 0, jnp.where(low_wall, -1 - reach, 0), reach)
    beyond = spot - 13
    high = jnp.where(
        beyond >= 0,
        jnp.where(high_wall, lanes - 1 - beyond, lanes - 1),
        lanes + beyond,
    )
    source = jnp.where(spot < 8, low, high)
    mirrored = ((spot < 3) & low_wall) | ((spot > 12) & high_wall)
    sign = jnp.where(mirrored, -1.0, 1.0)
    group = lane // width

    def gather(values, index):
        return jnp.take_along_axis(values, index, axis=1)

    def z_edge(x, _):
        for r in range(NVAR):
            value = gather(own(r, x), source)
            if r == NS + 2:
                value = value * sign
            edge_ref[r] = jnp.where(group == x, value, edge_ref[r])
        return 0

    def roll(values, shift):
        return values if shift % lanes == 0 else pltpu.roll(values, shift % lanes, 1)

    def z_split(u, i):
        fill_split(u, i, 2, alphas[2], prim_ref, up_ref, down_ref)
        for k in range(NVAR + 1):
            dup_ref[k, i] = roll(up_ref[k, i], -1) - up_ref[k, i]
            ddown_ref[k, i] = roll(down_ref[k, i], -1) - down_ref[k, i]

    def z_own(x, _):
        u = [own(r, x) for r in range(NVAR)]
        z_split(u, x + 3)
        return 0

    def z_faces(x, _):
        i = jnp.where(x == 8, 14, x + 3)

        def linear(r):
            here = up_ref[r, i] + roll(down_ref[r, i], -1)
            ahead = dup_ref[r, i] - ddown_ref[r, i]
            return 6.0 * here + (ahead + ahead) + (
                roll(dup_ref[r, i], 1) - roll(ddown_ref[r, i], -1)
            )

        def mean(q):
            value = prim_ref[q, i]
            return 0.5 * (value + roll(value, -1))

        def put(r, value):
            fz_ref[r, x] = value

        face(
            2,
            lambda r, k: roll(dup_ref[r, i], 2 - k),
            lambda r, k: roll(ddown_ref[r, i], k - 2),
            mean,
            linear,
            put,
        )
        return 0

    def x_prims(x, best):
        u = [own(r, x) for r in range(NVAR)]
        fill_cells(u, x + 3, table_ref, prim_ref)
        sound = prim_ref[SOUND, x + 3]
        return tuple(
            jnp.maximum(b, jnp.abs(prim_ref[VEL + d, x + 3]) + sound) for d, b in enumerate(best)
        )

    zero = jnp.zeros(tile, jnp.float32)
    best = lax.fori_loop(0, 8, x_prims, (zero, zero, zero))
    best = [jnp.max(b, axis=(0, 1), keepdims=True) for b in best]
    row = lax.broadcasted_iota(jnp.int32, tile, 0)
    value = jnp.where(row == 0, best[0], jnp.where(row == 1, best[1], best[2]))

    def fill_turned():
        lax.fori_loop(0, 8, y_prims, 0)

    def fill_edge():
        for r in range(NVAR):
            edge_ref[r] = zero
        lax.fori_loop(0, 8, z_edge, 0)
        fill_cells([edge_ref[r] for r in range(NVAR)], 14, table_ref, prim_ref)

    for n, along, held, slots, recv, base, meanwhile in (
        (size_y, along_y, mine_ref, slots_y, recv_y, 0, fill_edge),
        (size_x, along_x, line_ref, slots_x, recv_x, size_y, fill_turned),
    ):
        held[...] = value
        copies = []
        for offset in range(1, n):
            copy = pltpu.make_async_remote_copy(
                src_ref=held,
                dst_ref=slots.at[offset],
                send_sem=small_send.at[base + offset],
                recv_sem=recv.at[offset],
                device_id=along(offset),
                device_id_type=MESH,
            )
            copy.start()
            copies.append(copy)
        meanwhile()
        for offset, copy in enumerate(copies, 1):
            copy.wait()
            value = jnp.maximum(value, slots[offset])
    alphas = [jnp.broadcast_to(value[d : d + 1], tile) for d in range(3)]

    z_split([edge_ref[r] for r in range(NVAR)], 14)
    lax.fori_loop(0, 8, z_own, 0)
    lax.fori_loop(0, 9, z_faces, 0)

    split_own(1, turn_ref, turned)
    halos[2].wait()
    halos[3].wait()
    cells_halo(1, turn_ref, y_halo_tile)
    differences(13)
    faces_across(1, turn_ref, fx_ref)

    def y_rate(y, _):
        for r in range(NVAR):
            acc_ref[pl.ds(r * block + y, 8, stride=8), :] = fx_ref[r, y + 1] - fx_ref[r, y]
        return 0

    lax.fori_loop(0, 8, y_rate, 0)

    split_own(0, prim_ref, own)
    halos[0].wait()
    halos[1].wait()
    cells_halo(0, prim_ref, lambda side, r, k: hx_ref[side, r, k])
    differences(13)
    faces_across(0, prim_ref, fx_ref)

    scale = (-COURANT / 6.0) / (alphas[0] + alphas[1] + alphas[2])
    near = jnp.where(lane < 2, lane + 3, lane - lanes + 13)
    patched = (lane < 2) | (lane > lanes - 4)

    def finish(x, _):
        first = jnp.clip(width * x + near, 0, lanes - 1)
        below = jnp.full(tile, width * x + 2, jnp.int32)
        for r in range(NVAR):
            edges = fz_ref[r, 8]
            upper = jnp.where(patched, gather(edges, first), fz_ref[r, x])
            lower = jnp.where(lane == 0, gather(edges, below), roll(upper, 1))
            rows = pl.ds(pl.multiple_of(r * block + x * 8, 8), 8)
            rate = (upper - lower) + (fx_ref[r, x + 1] - fx_ref[r, x]) + acc_ref[rows, :]
            out_ref[rows, :] = scale * rate
        return 0

    lax.fori_loop(0, 8, finish, 0)


def shards(preserved_vector, nasa_table, gas_constant, species_index, face_kind):
    _, nx, ny, lanes = preserved_vector.shape
    size_x, size_y = lax.axis_size("gx"), lax.axis_size("gy")
    flat = preserved_vector.reshape(NVAR * nx * ny, lanes)
    smem = pl.BlockSpec(memory_space=pltpu.SMEM)
    anywhere = pl.BlockSpec(memory_space=pl.ANY)
    dma = pltpu.SemaphoreType.DMA

    def buffer(*shape):
        return pltpu.VMEM(shape + (8, lanes), jnp.float32)

    out = pl.pallas_call(
        functools.partial(fused, size_x, size_y),
        out_shape=jax.ShapeDtypeStruct(flat.shape, jnp.float32),
        in_specs=[smem] * 4 + [anywhere] * 3,
        out_specs=pl.BlockSpec(memory_space=pltpu.VMEM),
        scratch_shapes=[
            pltpu.VMEM(flat.shape, jnp.float32),
            buffer(2, NVAR, 3),
            pltpu.VMEM((2, NVAR, nx, 3, 1, lanes), jnp.float32),
            buffer(),
            buffer(),
            buffer(size_y),
            buffer(size_x),
            buffer(TABLE),
            buffer(PRIMS + 1, 15),
            buffer(PRIMS + 1, 15),
            buffer(NVAR + 1, 15),
            buffer(NVAR + 1, 15),
            buffer(NVAR + 1, 15),
            buffer(NVAR + 1, 15),
            buffer(NVAR, 9),
            buffer(NVAR, 9),
            pltpu.VMEM(flat.shape, jnp.float32),
            buffer(NVAR),
            dma(()),
            dma((size_x + size_y,)),
            dma((size_y,)),
            dma((size_x,)),
            dma((4,)),
            dma((4,)),
        ],
        compiler_params=pltpu.CompilerParams(collective_id=0, has_side_effects=True),
        name="increment",
    )(
        nasa_table.T, gas_constant, species_index, face_kind.reshape(2), flat,
        preserved_vector, preserved_vector.reshape(NVAR, nx, ny, 1, lanes),
    )
    return out.reshape(preserved_vector.shape)


def solution(mesh):
    return jax.shard_map(
        shards,
        mesh=mesh,
        in_specs=(P(None, "gx", "gy", None), P(), P(), P(), P("gx", "gy", None)),
        out_specs=P(None, "gx", "gy", None),
        check_vma=False,
    )
```

```python
import functools

import jax
import jax.numpy as jnp
from jax import lax
from jax.experimental import pallas as pl
from jax.experimental.pallas import tpu as pltpu
from jax.sharding import PartitionSpec as P

NS = 9
NVAR = 14
EPSILON = 1e-06
COURANT = 0.8
TOTAL = NVAR
PRIMS = 24
VEL, PASSIVE, GAMMA, SOUND, SLOPES = 9, 12, 13, 14, 15
TABLE = 7 * NS


def fill_table(nasa_ref, gas_ref, index_ref, table_ref):
    for i in range(NS):
        row = index_ref[i]
        gas = gas_ref[row]
        values = [
            gas,
            gas * nasa_ref[5, row],
            gas * (nasa_ref[0, row] - 1.0),
            gas * nasa_ref[1, row] * (1.0 / 2.0),
            gas * nasa_ref[2, row] * (1.0 / 3.0),
            gas * nasa_ref[3, row] * (1.0 / 4.0),
            gas * nasa_ref[4, row] * (1.0 / 5.0),
        ]
        for n, value in enumerate(values):
            table_ref[n * NS + i] = jnp.full(table_ref.shape[1:], value, jnp.float32)


def tree(terms):
    terms = list(terms)
    while len(terms) > 1:
        terms = [a + b for a, b in zip(terms[::2], terms[1::2])] + (
            [terms[-1]] if len(terms) % 2 else []
        )
    return terms[0]


def thermo(u, table_ref):
    rho = tree(u[:NS])
    inverse = 1.0 / rho
    vel = [m * inverse for m in u[NS : NS + 3]]
    square = tree([v * v for v in vel])
    inner = u[NS + 3] - 0.5 * tree([v * m for v, m in zip(vel, u[NS : NS + 3])])
    mix = [tree([u[i] * table_ref[n * NS + i] for i in range(NS)]) for n in range(7)]
    gas, m6, m1, m2, m3, m4, m5 = mix
    c2, c3, c4, c5 = 2.0 * m2, 3.0 * m3, 4.0 * m4, 5.0 * m5
    temp = 1.0 - (tree([m6, m1, m2, m3, m4, m5]) - inner) / tree([m1, c2, c3, c4, c5])

    def heat(t):
        return m1 + t * (c2 + t * (c3 + t * (c4 + t * c5)))

    energy = m6 + temp * (m1 + temp * (m2 + temp * (m3 + temp * (m4 + temp * m5))))
    temp = temp - (energy - inner) / heat(temp)
    pressure = temp * gas
    gamma = gas / heat(temp)
    sound = jnp.sqrt((1.0 + gamma) * pressure * inverse)
    return inverse, vel, square, temp, pressure, gamma, sound


def slopes_of(temp, gamma, square, table_ref):
    kinetic = 0.5 * gamma * square
    result = []
    for i in range(NS):
        k = [table_ref[n * NS + i] for n in range(7)]
        e = k[1] + temp * (k[2] + temp * (k[3] + temp * (k[4] + temp * (k[5] + temp * k[6]))))
        result.append(k[0] * temp - gamma * e + kinetic)
    return result


def reciprocal(x):
    return pl.reciprocal(x, approx=True)


def correction(d):
    d0, d1, d2, d3 = d
    e0, e1, e2 = d1 - d0, d2 - d1, d3 - d2
    h1, h2 = 0.75 * d1, 0.75 * d2
    near, far = h1 * d1 + 0.75 * EPSILON, h2 * d2 + 0.75 * EPSILON
    r0 = reciprocal(e0 * (e0 + h1) + near)
    r1 = reciprocal(e1 * (e1 + h1) + near)
    r2 = reciprocal(e2 * (e2 - h2) + far)
    a = r0 * r0 * (1.0 / 3.0)
    b = r1 * r1
    c = r2 * r2
    g0, g2 = e0 - e1, e1 - e2
    return (a * (g0 + g0) + c * g2) * reciprocal(a + c + (b + b))


def face(normal, up, down, mean, linear, put):
    phi = [mean(SLOPES + i) for i in range(NS)]
    vel = [mean(VEL + i) for i in range(3)]
    gamma, sound = mean(GAMMA), mean(SOUND)
    inv = 1.0 / sound
    inv2, half_inv = inv * inv, 0.5 * inv
    tangents = [t for t in range(3) if t != normal]
    sigma, slow, fast = ([], []), ([], []), ([], [])
    shear = [([], []), ([], [])]
    for side, get in enumerate((up, down)):
        for k in range(4):
            s = get(TOTAL, k)
            m = [get(NS + i, k) for i in range(3)]
            dp = tree([phi[i] * get(i, k) for i in range(NS)]) + gamma * (
                get(NS + 3, k) - tree([vel[i] * m[i] for i in range(3)])
            )
            scaled = dp * inv2
            jump = (m[normal] - vel[normal] * s) * half_inv
            half = 0.5 * scaled
            sigma[side].append(scaled)
            slow[side].append(half - jump)
            fast[side].append(half + jump)
            for n, t in enumerate(tangents):
                shear[n][side].append(m[t] - vel[t] * s)

    def both(pair):
        return correction(pair[0]) - correction(pair[1])

    slower, faster = both(slow), both(fast)
    shears = [both(pair) for pair in shear]
    acoustic = slower + faster
    total, weighted, blend = None, None, None
    for i in range(NS):
        y = mean(i)
        amp = both(
            (
                [up(i, k) - y * sigma[0][k] for k in range(4)],
                [down(i, k) - y * sigma[1][k] for k in range(4)],
            )
        )
        put(i, linear(i) + y * acoustic + amp)
        total = amp if i == 0 else total + amp
        weighted = phi[i] * amp if i == 0 else weighted + phi[i] * amp
        blend = phi[i] * y if i == 0 else blend + phi[i] * y
    z = mean(PASSIVE)
    amp = both(
        (
            [up(NS + 4, k) - z * sigma[0][k] for k in range(4)],
            [down(NS + 4, k) - z * sigma[1][k] for k in range(4)],
        )
    )
    put(NS + 4, linear(NS + 4) + z * acoustic + amp)
    mass = acoustic + total
    swing = sound * (faster - slower)
    put(NS + normal, linear(NS + normal) + vel[normal] * mass + swing)
    for n, t in enumerate(tangents):
        put(NS + t, linear(NS + t) + vel[t] * mass + shears[n])
    square = tree([v * v for v in vel])
    energy = (
        square * mass
        + ((sound * sound - blend) * acoustic - weighted) / gamma
        + vel[normal] * swing
        + vel[tangents[0]] * shears[0]
        + vel[tangents[1]] * shears[1]
    )
    put(NS + 3, linear(NS + 3) + energy)


def fill_cells(u, i, table_ref, prim_ref):
    inverse, vel, square, temp, pressure, gamma, sound = thermo(u, table_ref)
    for k in range(NS):
        prim_ref[k, i] = u[k] * inverse
    for k in range(3):
        prim_ref[VEL + k, i] = vel[k]
    prim_ref[PASSIVE, i] = u[NS + 4] * inverse
    prim_ref[GAMMA, i] = gamma
    prim_ref[SOUND, i] = sound
    for k, value in enumerate(slopes_of(temp, gamma, square, table_ref)):
        prim_ref[SLOPES + k, i] = value
    prim_ref[PRIMS, i] = pressure


def fill_split(u, i, normal, alpha, prim_ref, up_ref, down_ref):
    speed = prim_ref[VEL + normal, i]
    push = 0.5 * prim_ref[PRIMS, i]
    half = 0.5 * speed
    lean = 0.5 * alpha
    plus, minus = half + lean, half - lean
    for ref, factor in ((up_ref, plus), (down_ref, minus)):
        for k in range(NVAR):
            value = u[k] * factor
            if k == NS + normal:
                value = value + push
            if k == NS + 3:
                value = value + push * speed
            ref[k, i] = value
        ref[TOTAL, i] = tree(u[:NS]) * factor


MESH = pl.DeviceIdType.MESH


def fused(
    size_x, size_y,
    nasa_ref, gas_ref, index_ref, kind_ref, flat_ref, planes_ref, source_ref, out_ref,
    x_ref, hx_ref, hy_ref, mine_ref, line_ref, slots_y, slots_x,
    table_ref, prim_ref, turn_ref, up_ref, down_ref, dup_ref, ddown_ref,
    fx_ref, fz_ref, acc_ref, edge_ref, fy_ref, s0_ref, s1_ref, s2_ref, s3_ref,
    load_sem, small_send, recv_y, recv_x, big_send, big_recv,
):
    load = pltpu.make_async_copy(flat_ref, x_ref, load_sem)
    load.start()
    gx, gy = lax.axis_index("gx"), lax.axis_index("gy")
    nx, ny = planes_ref.shape[1], planes_ref.shape[2]

    def along_x(offset):
        return (lax.rem(gx + offset, size_x), gy)

    def along_y(offset):
        return (gx, lax.rem(gy + offset, size_y))

    barrier = pltpu.get_barrier_semaphore()
    for n, along in ((size_x, along_x), (size_y, along_y)):
        for offset in range(1, n):
            pl.semaphore_signal(barrier, inc=1, device_id=along(offset), device_id_type=MESH)
    fill_table(nasa_ref, gas_ref, index_ref, table_ref)
    pl.semaphore_wait(barrier, size_x + size_y - 2)

    halos = []
    for n, (source, target, device) in enumerate(
        (
            (planes_ref.at[:, pl.ds(nx - 3, 3)], hx_ref.at[0], along_x(1)),
            (planes_ref.at[:, pl.ds(0, 3)], hx_ref.at[1], along_x(size_x - 1)),
            (source_ref.at[:, :, pl.ds(ny - 3, 3)], hy_ref.at[0], along_y(1)),
            (source_ref.at[:, :, pl.ds(0, 3)], hy_ref.at[1], along_y(size_y - 1)),
        )
    ):
        copy = pltpu.make_async_remote_copy(
            src_ref=source,
            dst_ref=target,
            send_sem=big_send.at[n],
            recv_sem=big_recv.at[n],
            device_id=device,
            device_id_type=MESH,
        )
        copy.start()
        halos.append(copy)
    load.wait()

    lanes = x_ref.shape[1]
    tile = (8, lanes)
    block = nx * ny

    def own(r, x):
        return x_ref[pl.ds(pl.multiple_of(r * block + x * 8, 8), 8), :]

    def turned(r, y):
        return x_ref[pl.ds(r * block + y, 8, stride=8), :]

    def differences(first, last, split):
        up_ref, down_ref, dup_ref, ddown_ref = split

        def step(i, _):
            for k in range(NVAR + 1):
                dup_ref[k, i] = up_ref[k, i + 1] - up_ref[k, i]
                ddown_ref[k, i] = down_ref[k, i + 1] - down_ref[k, i]
            return 0

        lax.fori_loop(first, last, step, 0)

    def faces_across(normal, first, last, prim_ref, split, flux_ref):
        up_ref, down_ref, dup_ref, ddown_ref = split

        def step(i, _):
            def linear(r):
                here = up_ref[r, i + 2] + down_ref[r, i + 3]
                ahead = dup_ref[r, i + 2] - ddown_ref[r, i + 2]
                return 6.0 * here + (ahead + ahead) + (dup_ref[r, i + 1] - ddown_ref[r, i + 3])

            def put(r, value):
                flux_ref[r, i] = value

            face(
                normal,
                lambda r, k: dup_ref[r, i + k],
                lambda r, k: ddown_ref[r, i + 4 - k],
                lambda q: 0.5 * (prim_ref[q, i + 2] + prim_ref[q, i + 3]),
                linear,
                put,
            )
            return 0

        lax.fori_loop(first, last, step, 0)

    def y_halo_tile(side, r, k):
        return hy_ref[side, r, :, k, 0, :]

    def cells_halo(normal, prims, split, read):
        def step(k, _):
            for side, base in ((0, 0), (1, 11)):
                u = [read(side, r, k) for r in range(NVAR)]
                fill_cells(u, k + base, table_ref, prims)
                fill_split(u, k + base, normal, alphas[normal], prims, *split[:2])
            return 0

        lax.fori_loop(0, 3, step, 0)

    def split_own(normal, prims, split, read):
        def step(n, _):
            u = [read(r, n) for r in range(NVAR)]
            fill_split(u, n + 3, normal, alphas[normal], prims, *split[:2])
            return 0

        lax.fori_loop(0, 8, step, 0)

    def y_prims(y, _):
        fill_cells([turned(r, y) for r in range(NVAR)], y + 3, table_ref, turn_ref)
        return 0

    lane = lax.broadcasted_iota(jnp.int32, tile, 1)

    width = 16
    spot = lane % width
    reach = spot - 3
    low_wall, high_wall = kind_ref[0] == 1, kind_ref[1] == 1
    low = jnp.where(reach < 0, jnp.where(low_wall, -1 - reach, 0), reach)
    beyond = spot - 13
    high = jnp.where(
        beyond >= 0,
        jnp.where(high_wall, lanes - 1 - beyond, lanes - 1),
        lanes + beyond,
    )
    source = jnp.where(spot < 8, low, high)
    mirrored = ((spot < 3) & low_wall) | ((spot > 12) & high_wall)
    sign = jnp.where(mirrored, -1.0, 1.0)
    group = lane // width

    def gather(values, index):
        return jnp.take_along_axis(values, index, axis=1)

    def z_edge(x, _):
        for r in range(NVAR):
            value = gather(own(r, x), source)
            if r == NS + 2:
                value = value * sign
            edge_ref[r] = jnp.where(group == x, value, edge_ref[r])
        return 0

    def roll(values, shift):
        return values if shift % lanes == 0 else pltpu.roll(values, shift % lanes, 1)

    def z_split(u, i):
        fill_split(u, i, 2, alphas[2], prim_ref, up_ref, down_ref)
        for k in range(NVAR + 1):
            dup_ref[k, i] = roll(up_ref[k, i], -1) - up_ref[k, i]
            ddown_ref[k, i] = roll(down_ref[k, i], -1) - down_ref[k, i]

    def z_own(x, _):
        u = [own(r, x) for r in range(NVAR)]
        z_split(u, x + 3)
        return 0

    def z_faces(x, _):
        i = jnp.where(x == 8, 14, x + 3)

        def linear(r):
            here = up_ref[r, i] + roll(down_ref[r, i], -1)
            ahead = dup_ref[r, i] - ddown_ref[r, i]
            return 6.0 * here + (ahead + ahead) + (
                roll(dup_ref[r, i], 1) - roll(ddown_ref[r, i], -1)
            )

        def mean(q):
            value = prim_ref[q, i]
            return 0.5 * (value + roll(value, -1))

        def put(r, value):
            fz_ref[r, x] = value

        face(
            2,
            lambda r, k: roll(dup_ref[r, i], 2 - k),
            lambda r, k: roll(ddown_ref[r, i], k - 2),
            mean,
            linear,
            put,
        )
        return 0

    def x_prims(x, best):
        u = [own(r, x) for r in range(NVAR)]
        fill_cells(u, x + 3, table_ref, prim_ref)
        sound = prim_ref[SOUND, x + 3]
        return tuple(
            jnp.maximum(b, jnp.abs(prim_ref[VEL + d, x + 3]) + sound) for d, b in enumerate(best)
        )

    zero = jnp.zeros(tile, jnp.float32)
    best = lax.fori_loop(0, 8, x_prims, (zero, zero, zero))
    best = [jnp.max(b, axis=(0, 1), keepdims=True) for b in best]
    row = lax.broadcasted_iota(jnp.int32, tile, 0)
    value = jnp.where(row == 0, best[0], jnp.where(row == 1, best[1], best[2]))

    def fill_turned():
        lax.fori_loop(0, 8, y_prims, 0)

    def fill_edge():
        for r in range(NVAR):
            edge_ref[r] = zero
        lax.fori_loop(0, 8, z_edge, 0)
        fill_cells([edge_ref[r] for r in range(NVAR)], 14, table_ref, prim_ref)

    for n, along, held, slots, recv, base, meanwhile in (
        (size_y, along_y, mine_ref, slots_y, recv_y, 0, fill_edge),
        (size_x, along_x, line_ref, slots_x, recv_x, size_y, fill_turned),
    ):
        held[...] = value
        copies = []
        for offset in range(1, n):
            copy = pltpu.make_async_remote_copy(
                src_ref=held,
                dst_ref=slots.at[offset],
                send_sem=small_send.at[base + offset],
                recv_sem=recv.at[offset],
                device_id=along(offset),
                device_id_type=MESH,
            )
            copy.start()
            copies.append(copy)
        meanwhile()
        for offset, copy in enumerate(copies, 1):
            copy.wait()
            value = jnp.maximum(value, slots[offset])
    alphas = [jnp.broadcast_to(value[d : d + 1], tile) for d in range(3)]

    z_split([edge_ref[r] for r in range(NVAR)], 14)
    lax.fori_loop(0, 8, z_own, 0)
    lax.fori_loop(0, 9, z_faces, 0)

    splits = (up_ref, down_ref, dup_ref, ddown_ref), (s0_ref, s1_ref, s2_ref, s3_ref)
    plans = (
        (1, turn_ref, splits[1], turned, y_halo_tile, fy_ref, halos[2:]),
        (0, prim_ref, splits[0], own, lambda side, r, k: hx_ref[side, r, k], fx_ref, halos[:2]),
    )
    for normal, prims, split, read, _, flux, _ in plans:
        split_own(normal, prims, split, read)
        differences(3, 10, split)
        faces_across(normal, 3, 6, prims, split, flux)
    for normal, prims, split, _, read, flux, copies in plans:
        for copy in copies:
            copy.wait()
        cells_halo(normal, prims, split, read)
        differences(0, 3, split)
        differences(10, 13, split)
        faces_across(normal, 0, 3, prims, split, flux)
        faces_across(normal, 6, 9, prims, split, flux)

    def y_rate(y, _):
        for r in range(NVAR):
            acc_ref[pl.ds(r * block + y, 8, stride=8), :] = fy_ref[r, y + 1] - fy_ref[r, y]
        return 0

    lax.fori_loop(0, 8, y_rate, 0)

    scale = (-COURANT / 6.0) / (alphas[0] + alphas[1] + alphas[2])
    near = jnp.where(lane < 2, lane + 3, lane - lanes + 13)
    patched = (lane < 2) | (lane > lanes - 4)

    def finish(x, _):
        first = jnp.clip(width * x + near, 0, lanes - 1)
        below = jnp.full(tile, width * x + 2, jnp.int32)
        for r in range(NVAR):
            edges = fz_ref[r, 8]
            upper = jnp.where(patched, gather(edges, first), fz_ref[r, x])
            lower = jnp.where(lane == 0, gather(edges, below), roll(upper, 1))
            rows = pl.ds(pl.multiple_of(r * block + x * 8, 8), 8)
            rate = (upper - lower) + (fx_ref[r, x + 1] - fx_ref[r, x]) + acc_ref[rows, :]
            out_ref[rows, :] = scale * rate
        return 0

    lax.fori_loop(0, 8, finish, 0)


def shards(preserved_vector, nasa_table, gas_constant, species_index, face_kind):
    _, nx, ny, lanes = preserved_vector.shape
    size_x, size_y = lax.axis_size("gx"), lax.axis_size("gy")
    flat = preserved_vector.reshape(NVAR * nx * ny, lanes)
    smem = pl.BlockSpec(memory_space=pltpu.SMEM)
    anywhere = pl.BlockSpec(memory_space=pl.ANY)
    dma = pltpu.SemaphoreType.DMA

    def buffer(*shape):
        return pltpu.VMEM(shape + (8, lanes), jnp.float32)

    out = pl.pallas_call(
        functools.partial(fused, size_x, size_y),
        out_shape=jax.ShapeDtypeStruct(flat.shape, jnp.float32),
        in_specs=[smem] * 4 + [anywhere] * 3,
        out_specs=pl.BlockSpec(memory_space=pltpu.VMEM),
        scratch_shapes=[
            pltpu.VMEM(flat.shape, jnp.float32),
            buffer(2, NVAR, 3),
            pltpu.VMEM((2, NVAR, nx, 3, 1, lanes), jnp.float32),
            buffer(),
            buffer(),
            buffer(size_y),
            buffer(size_x),
            buffer(TABLE),
            buffer(PRIMS + 1, 15),
            buffer(PRIMS + 1, 15),
            buffer(NVAR + 1, 15),
            buffer(NVAR + 1, 15),
            buffer(NVAR + 1, 15),
            buffer(NVAR + 1, 15),
            buffer(NVAR, 9),
            buffer(NVAR, 9),
            pltpu.VMEM(flat.shape, jnp.float32),
            buffer(NVAR),
            buffer(NVAR, 9),
            *[buffer(NVAR + 1, 15) for _ in range(4)],
            dma(()),
            dma((size_x + size_y,)),
            dma((size_y,)),
            dma((size_x,)),
            dma((4,)),
            dma((4,)),
        ],
        compiler_params=pltpu.CompilerParams(collective_id=0, has_side_effects=True),
        name="increment",
    )(
        nasa_table.T, gas_constant, species_index, face_kind.reshape(2), flat,
        preserved_vector, preserved_vector.reshape(NVAR, nx, ny, 1, lanes),
    )
    return out.reshape(preserved_vector.shape)


def solution(mesh):
    return jax.shard_map(
        shards,
        mesh=mesh,
        in_specs=(P(None, "gx", "gy", None), P(), P(), P(), P("gx", "gy", None)),
        out_specs=P(None, "gx", "gy", None),
        check_vma=False,
    )
```
